32 devices in a mesh: pgroup: 8 (over y, x, core), tile: 4 (over z).
Axes of the slice: x: 2, y: 2, z: 4, core: 2. Of those that a mesh axis runs over, the one named last changes fastest.
Arguments:
- images: float32 [64, 256, 2048], P(('pgroup', 'tile')), may hold values from -6 to 6
- beams: float32 [64, 256, 2048], P(('pgroup', 'tile')), may hold values from 0.2 to 1
- row_block: int32 [64], P(('pgroup', 'tile')), may hold values from 0 to 14, as said below
- col_block: int32 [64], P(('pgroup', 'tile')), may hold values from 0 to 16
- band: int32 [64, 2], P(('pgroup', 'tile')), may hold values from 0 to 3
- row_frac: float32 [64], P(('pgroup', 'tile')), may hold values from 0.05 to 0.95
- col_frac: float32 [64], P(('pgroup', 'tile')), may hold values from 0.05 to 0.95
Outputs:
- numer: float32 [2048, 4096], P('tile', 'pgroup')
- weight: float32 [2048, 4096], P('tile', 'pgroup')
- normalised: float32 [2048, 4096], P('tile', 'pgroup')
The draws below stay inside these ranges and needn't reach their ends.
Inputs may be any that keep to these rules, and one draw needn't show every extreme that they name: With t = (p // 2) mod 4, row_block[p] - 4 t lies in 0 to 2, and the largest value is taken in every draw.
All inputs are finite; a program needn't handle non-finite values.
Results may differ from the reference program's by a relative error of at most 0.00002.
Values sent between devices are 32-bit elements; how exact they have to be, the bound alone decides.
A program may use at most 128 MiB of HBM per device.

```python
import math
import jax
import jax.numpy as jnp
from jax import lax

W = 2048
IMG_ROWS = 256
IMG_BLOCKS = 2
PTS_DEV = 2
POINTINGS = 64
TILE_BLOCKS = 4
SKY_ROWS = 2048
SKY_COLS = 4096
HALO = 4
N_TILE = 4


def draw_row_block(key, part):
    pointing = jnp.arange(POINTINGS, dtype=jnp.int32)
    owner = pointing // PTS_DEV % N_TILE
    offset = jax.random.randint(key, (POINTINGS,), 0, TILE_BLOCKS - IMG_BLOCKS + 1, dtype=jnp.int32)
    offset = offset.at[0].set(TILE_BLOCKS - IMG_BLOCKS)
    return owner * TILE_BLOCKS + offset


def place_ends(array, own_key, low, high):
    index_at = [jax.random.randint(jax.random.fold_in(own_key, axis), (), 0, length) for axis, length in enumerate(array.shape)]
    widest = array.shape.index(max(array.shape))
    next_to = index_at[:widest] + [(index_at[widest] + 1) % array.shape[widest]] + index_at[widest + 1:]
    return array.at[tuple(index_at)].set(low).at[tuple(next_to)].set(high)


def level_of(own_key, shape, shards, least, largest):
    factor_of = 1.0
    for dim, blocks in shards:
        draws = jax.random.uniform(jax.random.fold_in(jax.random.fold_in(own_key, 6), dim), (blocks,), jnp.float32, least / len(shards), largest / len(shards))
        factor_of = factor_of * jnp.repeat(jnp.exp(draws), shape[dim] // blocks).reshape((-1,) + (1,) * (len(shape) - 1 - dim))
    return factor_of


def centred(rng, dims, width, reach, cuts=(), kind=jnp.bfloat16):
    level = level_of(rng, dims, cuts, -0.22, 0.18) if cuts else 1.0
    entries = jax.random.normal(rng, dims, jnp.float32) * width * level
    return jnp.minimum(jnp.maximum(entries, -reach), reach).astype(kind)


def setup_inputs(seed: int = 0) -> dict:
    key_list = jax.random.split(jax.random.key(seed), 8)
    return {
        "images": centred(key_list[0], (POINTINGS, IMG_ROWS, W), 1.0, 6.0, ((0, 32),), jnp.float32),
        "beams": jnp.clip(jnp.exp(math.log(1.0) - 1.609438 * jax.random.uniform(key_list[1], (POINTINGS, IMG_ROWS, W), jnp.float32) ** level_of(key_list[1], (POINTINGS, IMG_ROWS, W), ((0, 32),), -0.2, 0.2)), 0.2, 1.0),
        "row_block": draw_row_block(jax.random.fold_in(key_list[7], 71), 0),
        "col_block": place_ends(jax.random.randint(key_list[3], (POINTINGS,), 0, (SKY_COLS - W) // 128 + 1), jax.random.fold_in(key_list[3], 1), 0, ((SKY_COLS - W) // 128 + 1) - 1).astype(jnp.int32),
        "band": place_ends(jax.random.randint(key_list[4], (POINTINGS, IMG_BLOCKS), 0, HALO), jax.random.fold_in(key_list[4], 1), 0, HALO - 1).astype(jnp.int32),
        "row_frac": jnp.clip(0.05 + 0.9 * jax.random.uniform(key_list[5], (POINTINGS,), jnp.float32) ** level_of(key_list[5], (POINTINGS,), ((0, 32),), -0.2, 0.2), 0.05, 0.95),
        "col_frac": jnp.clip(0.05 + 0.9 * jax.random.uniform(key_list[6], (POINTINGS,), jnp.float32) ** level_of(key_list[6], (POINTINGS,), ((0, 32),), -0.2, 0.2), 0.05, 0.95),
    }


def contribution(image_block, beam_block, shift, row_f, col_f):
    stacked = jnp.stack([beam_block * image_block, beam_block * beam_block])
    moved = jnp.concatenate([jnp.zeros_like(stacked[:, :, :1]), stacked[:, :, :-1]], axis=2)
    banded = (1.0 - col_f) * stacked + col_f * moved
    empty = jnp.zeros((2, 128 + HALO, banded.shape[2]), jnp.float32)
    zero = jnp.int32(0)
    first = lax.dynamic_update_slice(empty, (1.0 - row_f) * banded, (zero, shift.astype(jnp.int32), zero))
    second = lax.dynamic_update_slice(empty, row_f * banded, (zero, (shift + 1).astype(jnp.int32), zero))
    return first + second


def reference(images, beams, row_block, col_block, band, row_frac, col_frac):
    canvas = jnp.zeros((2, SKY_ROWS + 128 + HALO, SKY_COLS), jnp.float32)

    def visit(index, canvas):
        for block in range(IMG_BLOCKS):
            image_block = lax.dynamic_slice_in_dim(images[index], block * 128, 128, 0)
            beam_block = lax.dynamic_slice_in_dim(beams[index], block * 128, 128, 0)
            piece = contribution(image_block, beam_block, band[index, block], row_frac[index], col_frac[index])
            row_start = ((row_block[index] + block) * 128).astype(jnp.int32)
            col_start = (col_block[index] * 128).astype(jnp.int32)
            zero = jnp.int32(0)
            old = lax.dynamic_slice(canvas, (zero, row_start, col_start), piece.shape)
            canvas = lax.dynamic_update_slice(canvas, old + piece, (zero, row_start, col_start))
        return canvas

    canvas = lax.fori_loop(0, POINTINGS, visit, canvas)
    numer = canvas[0, :SKY_ROWS]
    weight = canvas[1, :SKY_ROWS]
    normalised = numer / jnp.maximum(weight, 0.05)
    return numer, weight, normalised
```

```python
import functools
import math

import jax
import jax.numpy as jnp
from jax import lax
from jax.experimental import pallas as pl
from jax.experimental.pallas import tpu as pltpu
from jax.sharding import PartitionSpec as P

TILE_BLOCKS = 4
SKY_COLS = 4096
LANES = 128
BLOCK = 128
PAD = 8
STEP = 64
START = 32
READY = START + PAD
EARLY = ((START, START), (START + STEP, STEP), (BLOCK, START))
MESH = pl.DeviceIdType.MESH
F32 = jnp.float32


def chip_grid(groups):
    chips = groups // 2
    along_x = math.isqrt(chips)
    while chips % along_x:
        along_x -= 1
    return chips // along_x, along_x


def kernel(
    ny, nx, n_tile,
    images, beams, row_block, col_block, band, row_frac, col_frac,
    numer, weight, normalised,
    raw, shaped, halo_out, halo_in, give, take, canvas,
    first_a, first_b, second_a, second_b,
    load_sem, halo_sem, swap_sem, first_sem, second_sem,
):
    points, img_rows, width = images.shape
    blocks = img_rows // BLOCK
    col_tiles = width // LANES
    sky_tiles = SKY_COLS // LANES
    sky_rows = TILE_BLOCKS * BLOCK
    own = sky_tiles // (ny * nx)
    half = own // 2
    per_core = sky_tiles // 2
    empty = 2 * points * blocks * col_tiles
    chunks = len(EARLY) + (TILE_BLOCKS - 1) * (BLOCK // STEP)

    me = lax.axis_index("pgroup")
    tile = lax.axis_index("tile")
    core = lax.rem(me, 2)
    chip = me // 2
    x = lax.rem(chip, nx)
    y = chip // nx
    partner = me + 1 - 2 * core
    x_peers = [(y * nx + lax.rem(x + d, nx)) * 2 + core for d in range(1, nx)]
    y_peers = [(lax.rem(y + d, ny) * nx + x) * 2 + core for d in range(1, ny)]
    counts = (nx, ny)
    places = (x, y)
    peers = (x_peers, y_peers)
    firsts = (first_a, first_b)
    seconds = (second_a, second_b)
    after = lax.rem(tile + 1, n_tile)
    before = lax.rem(tile + n_tile - 1, n_tile)

    pieces = [(img_rows - READY, READY), (img_rows - BLOCK, BLOCK - READY)]
    pieces += [(b * BLOCK, BLOCK) for b in reversed(range(blocks - 1))]
    loads = []
    for k, (low, size) in enumerate(pieces):
        for p in range(points):
            for which, source in enumerate((images, beams)):
                rows = pl.ds(low, size)
                copy = pltpu.make_async_copy(
                    source.at[p, rows], raw.at[which, p, rows], load_sem.at[which, p, k]
                )
                copy.start()
                loads.append((k, copy))

    barrier = pltpu.get_barrier_semaphore()
    near = [{"pgroup": q} for q in [partner] + x_peers + y_peers]
    near += [{"tile": after}, {"tile": before}]
    for device in near:
        pl.semaphore_signal(barrier, inc=1, device_id=device, device_id_type=MESH)

    def clear(index, _):
        shaped[index, :PAD] = jnp.zeros((PAD, LANES), F32)
        shaped[index, PAD + BLOCK :] = jnp.zeros((PAD, LANES), F32)
        return 0

    lax.fori_loop(0, empty, clear, 0, unroll=8)
    shaped[empty] = jnp.zeros((BLOCK + 2 * PAD, LANES), F32)

    first_lane = lax.broadcasted_iota(jnp.int32, (8, LANES), 1) == 0
    across = [(1.0 - col_frac[p], col_frac[p]) for p in range(points)]
    down = [(1.0 - row_frac[p], row_frac[p]) for p in range(points)]
    base_block = [row_block[p] - tile * TILE_BLOCKS for p in range(points)]
    base_tile = [col_block[p] for p in range(points)]

    def loaded(k):
        for at, copy in loads:
            if at == k:
                copy.wait()

    def interpolate(b, low, high):
        def one(r, _):
            source = pl.ds(pl.multiple_of(b * BLOCK + 8 * r, 8), 8)
            target = pl.ds(pl.multiple_of(PAD + 8 * r, 8), 8)
            for p in range(points):
                stay, go = across[p]
                prior = [jnp.zeros((8, LANES), F32)] * 2
                for t in range(col_tiles):
                    lanes = slice(t * LANES, (t + 1) * LANES)
                    beam = raw[1, p, source, lanes]
                    image = raw[0, p, source, lanes]
                    for a, here in enumerate((beam * image, beam * beam)):
                        turned = pltpu.roll(here, 1, 1)
                        moved = jnp.where(first_lane, prior[a], turned)
                        index = ((a * points + p) * blocks + b) * col_tiles + t
                        shaped[index, target] = stay * here + go * moved
                        prior[a] = turned
            return 0

        lax.fori_loop(low // 8, high // 8, one, 0)

    def sum_rows(a, sky_block, sky_tile, start, size):
        total = None
        for p in range(points):
            b = sky_block - base_block[p]
            t = sky_tile - base_tile[p]
            inside = (b >= 0) & (b < blocks) & (t >= 0) & (t < col_tiles)
            index = ((a * points + p) * blocks + b) * col_tiles + t
            index = jnp.where(inside, index, empty)
            shift = band[p, jnp.clip(b, 0, blocks - 1)]
            low = shaped[index, pl.ds(PAD + start - shift, size)]
            high = shaped[index, pl.ds(PAD - 1 + start - shift, size)]
            term = down[p][0] * low + down[p][1] * high
            total = term if total is None else total + term
        return total

    def sky_tile_of(a, which, slot):
        group = slot // half
        count = (ny, nx)[a]
        major, minor = group // count, lax.rem(group, count)
        at = minor * nx + major if a == 0 else major * nx + minor
        return at * own + which * half + lax.rem(slot, half)

    def block_of(a, d):
        size = per_core // counts[a]
        at = places[a] if d == 0 else lax.rem(places[a] + d, counts[a])
        return at * size, size

    def order():
        return [(a, d) for d in range(1, max(nx, ny)) for a in range(2) if d < counts[a]] + [(0, 0), (1, 0)]

    def chunk(m):
        if isinstance(m, int) and m < len(EARLY):
            below, size = EARLY[m]
            return pl.ds(sky_rows - below, size)
        start = sky_rows - BLOCK - STEP * (m - len(EARLY) + 1)
        return pl.ds(pl.multiple_of(start, STEP), STEP)

    def swap(m, a, d):
        first, size = block_of(a, d)
        view = (a, pl.ds(first, size), chunk(m))
        return pltpu.make_async_remote_copy(
            give.at[view], take.at[view], swap_sem.at[0, m, a, d], swap_sem.at[1, m, a, d],
            device_id={"pgroup": partner}, device_id_type=MESH,
        )

    def first_copy(m, a, d):
        first, size = block_of(a, d)
        rows = chunk(m)
        return pltpu.make_async_remote_copy(
            canvas.at[a, pl.ds(first, size), rows], firsts[a].at[d - 1, :, rows],
            first_sem.at[0, m, a, d - 1], first_sem.at[1, m, a, d - 1],
            device_id={"pgroup": peers[a][d - 1]}, device_id_type=MESH,
        )

    def second_copy(m, a, d):
        other = 1 - a
        first, _ = block_of(a, 0)
        at = lax.rem(places[other] + d, counts[other])
        rows = chunk(m)
        return pltpu.make_async_remote_copy(
            canvas.at[a, pl.ds(first + at * half, half), rows], seconds[a].at[d - 1, :, rows],
            second_sem.at[0, m, a, d - 1], second_sem.at[1, m, a, d - 1],
            device_id={"pgroup": peers[other][d - 1]}, device_id_type=MESH,
        )

    use = jnp.where(tile > 0, 1.0, 0.0)

    def put(target, a, which, slot, rows, sky_block, start, size, last, extra):
        sky_tile = sky_tile_of(a, which, slot)
        total = sum_rows(a, sky_block, sky_tile, start, size)
        if extra is not None:
            total = total + extra[a, slot, rows]
        target[a, slot, rows] = total
        if start == 0:
            top = total[:8] + sum_rows(a, sky_block - 1, sky_tile, BLOCK, 8)
            if last:
                top = top + use * halo_in[a, sky_tile]
            target[a, slot, pl.ds(rows.start, 8)] = top

    def build(m, sky_block, start, last=False):
        rows = chunk(m)
        for a, d in order():
            first, count = block_of(a, d)

            def one(s, _):
                put(give, a, 1 - core, first + s, rows, sky_block, start, rows.size, last, None)
                return 0

            lax.fori_loop(0, count, one, 0, unroll=2)
            swap(m, a, d).start()

    def combine(m, sky_block, start, last=False):
        rows = chunk(m)
        for a, d in order():
            first, count = block_of(a, d)
            swap(m, a, d).wait_recv()

            def one(s, _):
                put(canvas, a, core, first + s, rows, sky_block, start, rows.size, last, take)
                return 0

            lax.fori_loop(0, count, one, 0, unroll=2)
            if d:
                first_copy(m, a, d).start()

    halo = pltpu.make_async_remote_copy(
        halo_out, halo_in, halo_sem.at[0], halo_sem.at[1],
        device_id={"tile": after}, device_id_type=MESH,
    )

    def border(sky_tile, _):
        for a in range(2):
            halo_out[a, sky_tile] = sum_rows(a, TILE_BLOCKS - 1, sky_tile, BLOCK, 8)
        return 0

    top = TILE_BLOCKS - 1
    loaded(0)
    interpolate(blocks - 1, BLOCK - READY, BLOCK)
    pl.semaphore_wait(barrier, len(near))
    build(0, top, BLOCK - START)
    loaded(1)
    interpolate(blocks - 1, 0, BLOCK - READY)
    combine(0, top, BLOCK - START)
    build(1, top, START)
    for k, b in enumerate(reversed(range(blocks - 1))):
        loaded(2 + k)
        interpolate(b, 0, BLOCK)
    combine(1, top, START)
    build(2, top, 0)
    lax.fori_loop(0, sky_tiles, border, 0)
    halo.start()
    build(3, top - 1, STEP)
    combine(2, top, 0)

    def spread(i, _):
        at = top - 1 - i
        build(4 + 2 * i, at, 0)
        combine(3 + 2 * i, at, STEP)
        build(5 + 2 * i, at - 1, STEP)
        combine(4 + 2 * i, at, 0)
        return 0

    lax.fori_loop(0, top - 1, spread, 0)
    halo.wait_recv()
    build(chunks - 1, 0, 0, last=True)
    combine(chunks - 2, 0, STEP)
    combine(chunks - 1, 0, 0, last=True)

    def every(step):
        for m in range(len(EARLY)):
            step(m)

        def one(m, _):
            step(m)
            return 0

        lax.fori_loop(len(EARLY), chunks, one, 0)

    def middle(m):
        rows = chunk(m)
        for a in range(2):
            for d in range(1, counts[a]):
                first_copy(m, a, d).wait_recv()
            first, _ = block_of(a, 0)
            for e in range(1, counts[1 - a]):
                at = lax.rem(places[1 - a] + e, counts[1 - a]) * half

                def one(q, _):
                    total = canvas[a, first + at + q, rows]
                    for d in range(counts[a] - 1):
                        total = total + firsts[a][d, at + q, rows]
                    canvas[a, first + at + q, rows] = total
                    return 0

                lax.fori_loop(0, half, one, 0, unroll=True)
                second_copy(m, a, e).start()

    every(middle)

    def finish(m):
        rows = chunk(m)
        for a in range(2):
            for e in range(1, counts[1 - a]):
                second_copy(m, a, e).wait_recv()
        for q in range(half):
            sums = []
            for a in range(2):
                first, _ = block_of(a, 0)
                at = places[1 - a] * half + q
                total = canvas[a, first + at, rows]
                for d in range(counts[a] - 1):
                    total = total + firsts[a][d, at, rows]
                for e in range(counts[1 - a] - 1):
                    total = total + seconds[a][e, q, rows]
                sums.append(total)
            lanes = slice(q * LANES, (q + 1) * LANES)
            numer[rows, lanes] = sums[0]
            weight[rows, lanes] = sums[1]
            normalised[rows, lanes] = sums[0] / jnp.maximum(sums[1], 0.05)

    every(finish)

    def drain(m):
        for a in range(2):
            for d in range(counts[a]):
                swap(m, a, d).wait_send()
                if d:
                    first_copy(m, a, d).wait_send()
            for e in range(1, counts[1 - a]):
                second_copy(m, a, e).wait_send()

    every(drain)
    halo.wait_send()


def body(ny, nx, n_tile, images, beams, row_block, col_block, band, row_frac, col_frac):
    points, img_rows, width = images.shape
    blocks = img_rows // BLOCK
    col_tiles = width // LANES
    sky_tiles = SKY_COLS // LANES
    sky_rows = TILE_BLOCKS * BLOCK
    half = sky_tiles // (2 * ny * nx)
    per_core = sky_tiles // 2
    chunks = len(EARLY) + (TILE_BLOCKS - 1) * (BLOCK // STEP)
    own_cols = half * LANES
    most = max(nx, ny)
    dma = pltpu.SemaphoreType.DMA
    smem = pl.BlockSpec(memory_space=pltpu.SMEM)
    vmem = pl.BlockSpec(memory_space=pltpu.VMEM)
    out = pltpu.VMEM((sky_rows, own_cols), F32)
    numer, weight, normalised = pl.pallas_call(
        functools.partial(kernel, ny, nx, n_tile),
        out_shape=(out, out, out),
        in_specs=[pl.BlockSpec(memory_space=pl.ANY)] * 2 + [smem] * 5,
        out_specs=(vmem, vmem, vmem),
        scratch_shapes=[
            pltpu.VMEM((2, points, img_rows, width), F32),
            pltpu.VMEM((2 * points * blocks * col_tiles + 1, BLOCK + 2 * PAD, LANES), F32),
            pltpu.VMEM((2, sky_tiles, 8, LANES), F32),
            pltpu.VMEM((2, sky_tiles, 8, LANES), F32),
            pltpu.VMEM((2, per_core, sky_rows, LANES), F32),
            pltpu.VMEM((2, per_core, sky_rows, LANES), F32),
            pltpu.VMEM((2, per_core, sky_rows, LANES), F32),
            pltpu.VMEM((nx - 1, ny * half, sky_rows, LANES), F32),
            pltpu.VMEM((ny - 1, nx * half, sky_rows, LANES), F32),
            pltpu.VMEM((ny - 1, half, sky_rows, LANES), F32),
            pltpu.VMEM((nx - 1, half, sky_rows, LANES), F32),
            dma((2, points, blocks + 1)),
            dma((2,)),
            dma((2, chunks, 2, most)),
            dma((2, chunks, 2, most - 1)),
            dma((2, chunks, 2, most - 1)),
        ],
        compiler_params=pltpu.CompilerParams(
            collective_id=0, has_side_effects=True, vmem_limit_bytes=56 * 1024 * 1024
        ),
        name="combine",
    )(images, beams, row_block, col_block, band, row_frac, col_frac)
    return (numer, weight, normalised)


def solution(mesh):
    ny, nx = chip_grid(mesh.shape["pgroup"])
    return jax.shard_map(
        functools.partial(body, ny, nx, mesh.shape["tile"]),
        mesh=mesh,
        in_specs=(
            P(("pgroup", "tile"), None, None),
            P(("pgroup", "tile"), None, None),
            P(("pgroup", "tile")),
            P(("pgroup", "tile")),
            P(("pgroup", "tile"), None),
            P(("pgroup", "tile")),
            P(("pgroup", "tile")),
        ),
        out_specs=(P("tile", "pgroup"), P("tile", "pgroup"), P("tile", "pgroup")),
        check_vma=False,
    )
```

```python
import functools
import math

import jax
import jax.numpy as jnp
from jax import lax
from jax.experimental import pallas as pl
from jax.experimental.pallas import tpu as pltpu
from jax.sharding import PartitionSpec as P

TILE_BLOCKS = 4
SKY_COLS = 4096
LANES = 128
BLOCK = 128
PAD = 8
STEP = 64
START = 32
READY = START + PAD
FINE = 2
EARLY = ((START, START), (START + STEP, STEP), (BLOCK, START))
MESH = pl.DeviceIdType.MESH
F32 = jnp.float32


def chip_grid(groups):
    chips = groups // 2
    along_x = math.isqrt(chips)
    while chips % along_x:
        along_x -= 1
    return chips // along_x, along_x


def kernel(
    ny, nx, n_tile,
    images, beams, row_block_in, col_block_in, band_in, row_frac_in, col_frac_in,
    numer, weight, normalised,
    row_block, col_block, band, row_frac, col_frac,
    raw, shaped, halo_out, halo_in, give, take, canvas,
    first_a, first_b, second,
    small_sem, load_sem, halo_sem, entered, swap_sem, first_sem, second_sem, send_sem,
):
    points, img_rows, width = images.shape
    blocks = img_rows // BLOCK
    col_tiles = width // LANES
    sky_tiles = SKY_COLS // LANES
    sky_rows = TILE_BLOCKS * BLOCK
    own = sky_tiles // (ny * nx)
    half = own // 2
    per_core = sky_tiles // 2
    empty = points * blocks * col_tiles
    chunks = len(EARLY) + (TILE_BLOCKS - 1) * (BLOCK // STEP)

    me = lax.axis_index("pgroup")
    tile = lax.axis_index("tile")
    core = lax.rem(me, 2)
    chip = me // 2
    x = lax.rem(chip, nx)
    y = chip // nx
    partner = me + 1 - 2 * core
    x_peers = [(y * nx + lax.rem(x + d, nx)) * 2 + core for d in range(1, nx)]
    y_peers = [(lax.rem(y + d, ny) * nx + x) * 2 + core for d in range(1, ny)]
    counts = (nx, ny)
    most = max(nx, ny)
    places = (x, y)
    peers = (x_peers, y_peers)
    firsts = (first_a, first_b)
    seconds = (second.at[pl.ds(0, ny - 1)], second.at[pl.ds(ny - 1, nx - 1)])
    after = lax.rem(tile + 1, n_tile)
    before = lax.rem(tile + n_tile - 1, n_tile)

    pieces = [(img_rows - READY, READY), (img_rows - BLOCK, BLOCK - READY)]
    pieces += [(b * BLOCK, BLOCK) for b in reversed(range(blocks - 1))]
    for k, (low, size) in enumerate(pieces):
        for p in range(points):
            for which, source in enumerate((images, beams)):
                rows = pl.ds(low, size)
                pltpu.make_async_copy(
                    source.at[p, rows], raw.at[which, p, rows], load_sem.at[k]
                ).start()
        if k == 0:
            small = [
                pltpu.make_async_copy(source, target, small_sem.at[n])
                for n, (source, target) in enumerate((
                    (row_block_in, row_block), (col_block_in, col_block), (band_in, band),
                    (row_frac_in, row_frac), (col_frac_in, col_frac),
                ))
            ]
            for copy in small:
                copy.start()

    barrier = pltpu.get_barrier_semaphore()
    near = [partner] + x_peers + y_peers
    for q in near:
        pl.semaphore_signal(barrier, inc=1, device_id={"pgroup": q}, device_id_type=MESH)

    @pl.when(tile < n_tile - 1)
    def _():
        pl.semaphore_signal(barrier, inc=1, device_id={"tile": after}, device_id_type=MESH)

    def clear(index, _):
        for a in range(2):
            shaped[a, index, :PAD] = jnp.zeros((PAD, LANES), F32)
            shaped[a, index, PAD + BLOCK :] = jnp.zeros((PAD, LANES), F32)
        return 0

    lax.fori_loop(0, empty, clear, 0, unroll=8)
    for a in range(2):
        shaped[a, empty] = jnp.zeros((BLOCK + 2 * PAD, LANES), F32)
    for copy in small:
        copy.wait()

    first_lane = lax.broadcasted_iota(jnp.int32, (8, LANES), 1) == 0
    across = [(1.0 - col_frac[p], col_frac[p]) for p in range(points)]
    down = [(1.0 - row_frac[p], row_frac[p]) for p in range(points)]
    base_block = [row_block[p] - tile * TILE_BLOCKS for p in range(points)]
    base_tile = [col_block[p] for p in range(points)]

    def loaded(k):
        low, size = pieces[k]
        view = raw.at[:, :, pl.ds(low, size)]
        pltpu.make_async_copy(view, view, load_sem.at[k]).wait()

    def interpolate(b, low, high):
        def one(r, _):
            source = pl.ds(pl.multiple_of(b * BLOCK + 8 * r, 8), 8)
            target = pl.ds(pl.multiple_of(PAD + 8 * r, 8), 8)
            for p in range(points):
                stay, go = across[p]
                prior = [jnp.zeros((8, LANES), F32)] * 2
                for t in range(col_tiles):
                    lanes = slice(t * LANES, (t + 1) * LANES)
                    beam = raw[1, p, source, lanes]
                    image = raw[0, p, source, lanes]
                    for a, here in enumerate((beam * image, beam * beam)):
                        turned = pltpu.roll(here, 1, 1)
                        moved = jnp.where(first_lane, prior[a], turned)
                        shaped[a, (p * blocks + b) * col_tiles + t, target] = stay * here + go * moved
                        prior[a] = turned
            return 0

        lax.fori_loop(low // 8, high // 8, one, 0)

    def block_terms(sky_block):
        terms = []
        for p in range(points):
            b = sky_block - base_block[p]
            within = (b >= 0) & (b < blocks)
            b = jnp.clip(b, 0, blocks - 1)
            shift = band[p, b]
            at = jnp.where(within, base_tile[p], sky_tiles)
            terms.append((at, (p * blocks + b) * col_tiles - base_tile[p], PAD - shift))
        return terms

    def indices(terms, sky_tile):
        found = []
        for at, base, _ in terms:
            t = sky_tile - at
            found.append(jnp.where((t >= 0) & (t < col_tiles), base + sky_tile, empty))
        return found

    def sum_rows(a, terms, index, start, size):
        total = None
        for p in range(points):
            at = terms[p][2] + start
            low = shaped[a, index[p], pl.ds(at, size)]
            high = shaped[a, index[p], pl.ds(at - 1, size)]
            term = down[p][0] * low + down[p][1] * high
            total = term if total is None else total + term
        return total

    def slot_of(a, chip_at):
        if a == 1:
            return chip_at * half
        return (lax.rem(chip_at, nx) * ny + chip_at // nx) * half

    def block_of(a, d):
        size = per_core // counts[a]
        at = places[a] if d == 0 else lax.rem(places[a] + d, counts[a])
        return at * size, size

    def order():
        return [(a, d) for d in range(1, max(nx, ny)) for a in range(2) if d < counts[a]] + [(0, 0), (1, 0)]

    def chunk(m):
        if isinstance(m, int) and m < len(EARLY):
            below, size = EARLY[m]
            return pl.ds(sky_rows - below, size)
        start = sky_rows - BLOCK - STEP * (m - len(EARLY) + 1)
        return pl.ds(pl.multiple_of(start, STEP), STEP)

    def swap(m, a=None, d=None):
        if a is None:
            view = (slice(None), slice(None), chunk(m))
            sem = swap_sem.at[m + FINE * (2 * most - 1)]
        else:
            first, size = block_of(a, d)
            view = (a, pl.ds(first, size), chunk(m))
            sem = swap_sem.at[(m * 2 + a) * most + d]
        return pltpu.make_async_remote_copy(
            give.at[view], take.at[view], send_sem.at[0], sem,
            device_id={"pgroup": partner}, device_id_type=MESH,
        )

    def first_copy(m, a, d):
        first, size = block_of(a, d)
        rows = chunk(m)
        return pltpu.make_async_remote_copy(
            canvas.at[a, pl.ds(first, size), rows], firsts[a].at[d - 1, :, rows],
            send_sem.at[1 + a], first_sem.at[m, a],
            device_id={"pgroup": peers[a][d - 1]}, device_id_type=MESH,
        )

    def second_copy(m, a, d):
        other = 1 - a
        first, _ = block_of(a, 0)
        at = lax.rem(places[other] + d, counts[other])
        rows = chunk(m)
        return pltpu.make_async_remote_copy(
            canvas.at[a, pl.ds(first + at * half, half), rows], seconds[a].at[d - 1, :, rows],
            send_sem.at[3 + a], second_sem.at[m],
            device_id={"pgroup": peers[other][d - 1]}, device_id_type=MESH,
        )

    def arrived(view, sem):
        pltpu.make_async_copy(view, view, sem).wait()

    def put(target, a, slot, sky_tile, rows, start, terms, index, above, index_above, last, extra):
        total = sum_rows(a, terms, index, start, rows.size)
        if extra is not None:
            total = total + extra[a, slot, rows]
        target[a, slot, rows] = total
        if start == 0:
            top = total[:8] + sum_rows(a, above, index_above, BLOCK, 8)
            if last:
                top = top + halo_in[a, sky_tile]
            target[a, slot, pl.ds(rows.start, 8)] = top

    def cover(target, which, m, sky_block, start, arrays, chips, last, extra):
        rows = chunk(m)
        terms = block_terms(sky_block)
        above = block_terms(sky_block - 1) if start == 0 else None

        def one(n, _):
            chip_at = chips(n)
            for q in range(half):
                sky_tile = chip_at * own + which * half + q
                index = indices(terms, sky_tile)
                index_above = indices(above, sky_tile) if start == 0 else None
                for a in arrays:
                    put(
                        target, a, slot_of(a, chip_at) + q, sky_tile, rows, start,
                        terms, index, above, index_above, last, extra,
                    )
            return 0

        return one

    def part(target, which, m, sky_block, start, a, d, extra):
        at = places[a] if d == 0 else lax.rem(places[a] + d, counts[a])
        chips = (lambda n: n * nx + at) if a == 0 else (lambda n: at * nx + n)
        one = cover(target, which, m, sky_block, start, (a,), chips, False, extra)
        lax.fori_loop(0, counts[1 - a], one, 0)

    def build(m, sky_block, start, last=False):
        if isinstance(m, int) and m < FINE:
            for a, d in order():
                part(give, 1 - core, m, sky_block, start, a, d, None)
            return
        one = cover(give, 1 - core, m, sky_block, start, (0, 1), lambda n: n, last, None)
        lax.fori_loop(0, ny * nx, one, 0)
        swap(m).start()

    def offer(m):
        for a, d in order():
            swap(m, a, d).start()

    def combine(m, sky_block, start, last=False):
        if isinstance(m, int) and m < FINE:
            for a, d in order():
                swap(m, a, d).wait_recv()
                part(canvas, core, m, sky_block, start, a, d, take)
                if d:
                    first_copy(m, a, d).start()
            return
        swap(m).wait_recv()
        one = cover(canvas, core, m, sky_block, start, (0, 1), lambda n: n, last, take)
        lax.fori_loop(0, ny * nx, one, 0)
        for a, d in order():
            if d:
                first_copy(m, a, d).start()

    halo = pltpu.make_async_remote_copy(
        halo_out, halo_in, halo_sem.at[0], halo_sem.at[1],
        device_id={"tile": after}, device_id_type=MESH,
    )

    top = TILE_BLOCKS - 1
    top_terms = block_terms(top)

    def border(sky_tile, _):
        index = indices(top_terms, sky_tile)
        for a in range(2):
            halo_out[a, sky_tile] = sum_rows(a, top_terms, index, BLOCK, 8)
        return 0

    loaded(0)
    interpolate(blocks - 1, BLOCK - READY, BLOCK)
    build(0, top, BLOCK - START)
    pl.semaphore_wait(barrier, len(near) + jnp.where(tile > 0, 1, 0))
    offer(0)
    loaded(1)
    interpolate(blocks - 1, 0, BLOCK - READY)

    @pl.when(tile > 0)
    def _():
        pl.semaphore_signal(entered, inc=1, device_id={"tile": before}, device_id_type=MESH)

    @pl.when(tile == 0)
    def _():
        halo_in[...] = jnp.zeros(halo_in.shape, F32)

    combine(0, top, BLOCK - START)
    build(1, top, START)
    offer(1)
    for k, b in enumerate(reversed(range(blocks - 1))):
        loaded(2 + k)
        interpolate(b, 0, BLOCK)
    combine(1, top, START)
    build(2, top, 0)
    lax.fori_loop(0, sky_tiles, border, 0, unroll=4)

    @pl.when(tile < n_tile - 1)
    def _():
        pl.semaphore_wait(entered, 1)
        halo.start()

    build(3, top - 1, STEP)
    combine(2, top, 0)

    def spread(i, _):
        at = top - 1 - i
        build(4 + 2 * i, at, 0)
        combine(3 + 2 * i, at, STEP)
        build(5 + 2 * i, at - 1, STEP)
        combine(4 + 2 * i, at, 0)
        return 0

    lax.fori_loop(0, top - 1, spread, 0)

    @pl.when(tile > 0)
    def _():
        halo.wait_recv()

    build(chunks - 1, 0, 0, last=True)
    combine(chunks - 2, 0, STEP)
    combine(chunks - 1, 0, 0, last=True)

    def every(step):
        for m in range(len(EARLY)):
            step(m)

        def one(m, _):
            step(m)
            return 0

        lax.fori_loop(len(EARLY), chunks, one, 0)

    def middle(m):
        rows = chunk(m)
        for a in range(2):
            arrived(firsts[a].at[:, :, rows], first_sem.at[m, a])
            first, _ = block_of(a, 0)
            for e in range(1, counts[1 - a]):
                at = lax.rem(places[1 - a] + e, counts[1 - a]) * half

                def one(q, _):
                    total = canvas[a, first + at + q, rows]
                    for d in range(counts[a] - 1):
                        total = total + firsts[a][d, at + q, rows]
                    canvas[a, first + at + q, rows] = total
                    return 0

                lax.fori_loop(0, half, one, 0, unroll=True)
                second_copy(m, a, e).start()

    every(middle)

    def finish(m):
        rows = chunk(m)
        arrived(second.at[:, :, rows], second_sem.at[m])
        for q in range(half):
            sums = []
            for a in range(2):
                first, _ = block_of(a, 0)
                at = places[1 - a] * half + q
                total = canvas[a, first + at, rows]
                for d in range(counts[a] - 1):
                    total = total + firsts[a][d, at, rows]
                for e in range(counts[1 - a] - 1):
                    total = total + seconds[a][e, q, rows]
                sums.append(total)
            lanes = slice(q * LANES, (q + 1) * LANES)
            numer[rows, lanes] = sums[0]
            weight[rows, lanes] = sums[1]
            normalised[rows, lanes] = sums[0] / jnp.maximum(sums[1], 0.05)

    every(finish)

    arrived(give, send_sem.at[0])
    for a in range(2):
        arrived(firsts[a], send_sem.at[1 + a])
        arrived(seconds[a], send_sem.at[3 + a])

    @pl.when(tile < n_tile - 1)
    def _():
        halo.wait_send()


def copy_out(numer, weight, normalised, numer_out, weight_out, normalised_out, sem):
    pairs = ((numer, numer_out), (weight, weight_out), (normalised, normalised_out))
    copies = [pltpu.make_async_copy(a, b, sem.at[n]) for n, (a, b) in enumerate(pairs)]
    for copy in copies:
        copy.start()
    for copy in copies:
        copy.wait()


def body(ny, nx, n_tile, images, beams, row_block, col_block, band, row_frac, col_frac):
    points, img_rows, width = images.shape
    blocks = img_rows // BLOCK
    col_tiles = width // LANES
    sky_tiles = SKY_COLS // LANES
    sky_rows = TILE_BLOCKS * BLOCK
    half = sky_tiles // (2 * ny * nx)
    per_core = sky_tiles // 2
    chunks = len(EARLY) + (TILE_BLOCKS - 1) * (BLOCK // STEP)
    own_cols = half * LANES
    most = max(nx, ny)
    dma = pltpu.SemaphoreType.DMA
    anywhere = pl.BlockSpec(memory_space=pl.ANY)
    scalars = [pltpu.SMEM(v.shape, v.dtype) for v in (row_block, col_block, band, row_frac, col_frac)]
    vmem = pl.BlockSpec(memory_space=pltpu.VMEM)
    out = pltpu.VMEM((sky_rows, own_cols), F32)
    numer, weight, normalised = pl.pallas_call(
        functools.partial(kernel, ny, nx, n_tile),
        out_shape=(out, out, out),
        in_specs=[anywhere] * 7,
        out_specs=(vmem, vmem, vmem),
        scratch_shapes=scalars + [
            pltpu.VMEM((2, points, img_rows, width), F32),
            pltpu.VMEM((2, points * blocks * col_tiles + 1, BLOCK + 2 * PAD, LANES), F32),
            pltpu.VMEM((2, sky_tiles, 8, LANES), F32),
            pltpu.VMEM((2, sky_tiles, 8, LANES), F32),
            pltpu.VMEM((2, per_core, sky_rows, LANES), F32),
            pltpu.VMEM((2, per_core, sky_rows, LANES), F32),
            pltpu.VMEM((2, per_core, sky_rows, LANES), F32),
            pltpu.VMEM((nx - 1, ny * half, sky_rows, LANES), F32),
            pltpu.VMEM((ny - 1, nx * half, sky_rows, LANES), F32),
            pltpu.VMEM((ny - 1 + nx - 1, half, sky_rows, LANES), F32),
            dma((5,)),
            dma((blocks + 1,)),
            dma((2,)),
            pltpu.SemaphoreType.REGULAR,
            dma((chunks + FINE * (2 * most - 1),)),
            dma((chunks, 2)),
            dma((chunks,)),
            dma((5,)),
        ],
        compiler_params=pltpu.CompilerParams(
            collective_id=0, has_side_effects=True, vmem_limit_bytes=56 * 1024 * 1024
        ),
        name="combine",
    )(images, beams, row_block, col_block, band, row_frac, col_frac)
    flat = jax.ShapeDtypeStruct((sky_rows, own_cols), F32)
    return pl.pallas_call(
        copy_out,
        out_shape=(flat, flat, flat),
        in_specs=[vmem] * 3,
        out_specs=(anywhere,) * 3,
        scratch_shapes=[dma((3,))],
        name="copy_out",
    )(*[pltpu.with_memory_space_constraint(v, pltpu.VMEM) for v in (numer, weight, normalised)])


def solution(mesh):
    ny, nx = chip_grid(mesh.shape["pgroup"])
    return jax.shard_map(
        functools.partial(body, ny, nx, mesh.shape["tile"]),
        mesh=mesh,
        in_specs=(
            P(("pgroup", "tile"), None, None),
            P(("pgroup", "tile"), None, None),
            P(("pgroup", "tile")),
            P(("pgroup", "tile")),
            P(("pgroup", "tile"), None),
            P(("pgroup", "tile")),
            P(("pgroup", "tile")),
        ),
        out_specs=(P("tile", "pgroup"), P("tile", "pgroup"), P("tile", "pgroup")),
        check_vma=False,
    )
```

```python
import functools
import math

import jax
import jax.numpy as jnp
from jax import lax
from jax.experimental import pallas as pl
from jax.experimental.pallas import tpu as pltpu
from jax.sharding import PartitionSpec as P

TILE_BLOCKS = 4
SKY_COLS = 4096
LANES = 128
BLOCK = 128
PAD = 8
STEP = 64
START = 32
READY = START + PAD
PIECES = ((104, 128), (88, 104), (0, 88))
EARLY = ((16, 16), (32, 16), (64, 32), (BLOCK, STEP))
FINE = len(EARLY)
MESH = pl.DeviceIdType.MESH
F32 = jnp.float32


def chip_grid(groups):
    chips = groups // 2
    along_x = math.isqrt(chips)
    while chips % along_x:
        along_x -= 1
    return chips // along_x, along_x


def kernel(
    ny, nx, n_tile,
    images, beams, row_block_in, col_block_in, band_in, row_frac_in, col_frac_in,
    numer, weight, normalised,
    row_block, col_block, band, row_frac, col_frac,
    raw, shaped, halo_out, halo_in, give, take, canvas,
    inbox,
    small_sem, load_sem, halo_sem, entered, swap_sem, first_sem, second_sem, send_sem,
):
    points, img_rows, width = images.shape
    blocks = img_rows // BLOCK
    col_tiles = width // LANES
    sky_tiles = SKY_COLS // LANES
    sky_rows = TILE_BLOCKS * BLOCK
    own = sky_tiles // (ny * nx)
    half = own // 2
    per_core = sky_tiles // 2
    empty = points * blocks * col_tiles
    chunks = len(EARLY) + (TILE_BLOCKS - 1) * (BLOCK // STEP)

    me = lax.axis_index("pgroup")
    tile = lax.axis_index("tile")
    core = lax.rem(me, 2)
    chip = me // 2
    x = lax.rem(chip, nx)
    y = chip // nx
    partner = me + 1 - 2 * core
    x_peers = [(y * nx + lax.rem(x + d, nx)) * 2 + core for d in range(1, nx)]
    y_peers = [(lax.rem(y + d, ny) * nx + x) * 2 + core for d in range(1, ny)]
    counts = (nx, ny)
    most = max(nx, ny)
    places = (x, y)
    peers = (x_peers, y_peers)
    sizes = (per_core // nx, per_core // ny)
    offsets = (0, (nx - 1) * sizes[0])
    first_tiles = offsets[1] + (ny - 1) * sizes[1]
    second_tiles = (first_tiles, first_tiles + (ny - 1) * half)
    every_tile = second_tiles[1] + (nx - 1) * half
    after = lax.rem(tile + 1, n_tile)
    before = lax.rem(tile + n_tile - 1, n_tile)

    pieces = [(img_rows - BLOCK + low, high - low) for low, high in PIECES]
    pieces += [(b * BLOCK, BLOCK) for b in reversed(range(blocks - 1))]

    def load(k):
        low, size = pieces[k]
        for p in range(points):
            for which, source in enumerate((images, beams)):
                rows = pl.ds(low, size)
                pltpu.make_async_copy(
                    source.at[p, rows], raw.at[which, p, rows], load_sem.at[k]
                ).start()

    load(0)
    small = [
        pltpu.make_async_copy(source, target, small_sem.at[n])
        for n, (source, target) in enumerate((
            (row_block_in, row_block), (col_block_in, col_block), (band_in, band),
            (row_frac_in, row_frac), (col_frac_in, col_frac),
        ))
    ]
    for copy in small:
        copy.start()
    for k in range(1, len(pieces)):
        load(k)

    barrier = pltpu.get_barrier_semaphore()
    near = [partner] + x_peers + y_peers
    for q in near:
        pl.semaphore_signal(barrier, inc=1, device_id={"pgroup": q}, device_id_type=MESH)

    @pl.when(tile < n_tile - 1)
    def _():
        pl.semaphore_signal(barrier, inc=1, device_id={"tile": after}, device_id_type=MESH)

    def clear(index, _):
        for a in range(2):
            shaped[a, index, :PAD] = jnp.zeros((PAD, LANES), F32)
            shaped[a, index, PAD + BLOCK :] = jnp.zeros((PAD, LANES), F32)
        return 0

    lax.fori_loop(0, empty, clear, 0, unroll=8)
    for a in range(2):
        shaped[a, empty] = jnp.zeros((BLOCK + 2 * PAD, LANES), F32)
    for copy in small:
        copy.wait()

    first_lane = lax.broadcasted_iota(jnp.int32, (8, LANES), 1) == 0
    across = [(1.0 - col_frac[p], col_frac[p]) for p in range(points)]
    down = [(1.0 - row_frac[p], row_frac[p]) for p in range(points)]
    base_block = [row_block[p] - tile * TILE_BLOCKS for p in range(points)]
    base_tile = [col_block[p] for p in range(points)]

    def loaded(k):
        low, size = pieces[k]
        view = raw.at[:, :, pl.ds(low, size)]
        pltpu.make_async_copy(view, view, load_sem.at[k]).wait()

    def interpolate(b, low, high, unroll):
        def one(r, _):
            source = pl.ds(pl.multiple_of(b * BLOCK + 8 * r, 8), 8)
            target = pl.ds(pl.multiple_of(PAD + 8 * r, 8), 8)
            for p in range(points):
                stay, go = across[p]
                prior = [jnp.zeros((8, LANES), F32)] * 2
                for t in range(col_tiles):
                    lanes = slice(t * LANES, (t + 1) * LANES)
                    beam = raw[1, p, source, lanes]
                    image = raw[0, p, source, lanes]
                    for a, here in enumerate((beam * image, beam * beam)):
                        turned = pltpu.roll(here, 1, 1)
                        moved = jnp.where(first_lane, prior[a], turned)
                        shaped[a, (p * blocks + b) * col_tiles + t, target] = stay * here + go * moved
                        prior[a] = turned
            return 0

        lax.fori_loop(low // 8, high // 8, one, 0, unroll=unroll)

    def block_terms(sky_block):
        terms = []
        for p in range(points):
            b = sky_block - base_block[p]
            within = (b >= 0) & (b < blocks)
            b = jnp.clip(b, 0, blocks - 1)
            shift = band[p, b]
            at = jnp.where(within, base_tile[p], sky_tiles)
            terms.append((at, (p * blocks + b) * col_tiles - base_tile[p], PAD - shift))
        return terms

    def indices(terms, sky_tile):
        found = []
        for at, base, _ in terms:
            t = sky_tile - at
            found.append(jnp.where((t >= 0) & (t < col_tiles), base + sky_tile, empty))
        return found

    def sum_rows(a, terms, index, start, size):
        total = None
        for p in range(points):
            at = terms[p][2] + start
            low = shaped[a, index[p], pl.ds(at, size)]
            high = shaped[a, index[p], pl.ds(at - 1, size)]
            term = down[p][0] * low + down[p][1] * high
            total = term if total is None else total + term
        return total

    def slot_of(a, chip_at):
        if a == 1:
            return chip_at * half
        return (lax.rem(chip_at, nx) * ny + chip_at // nx) * half

    def place_of(a, d):
        return places[a] if d == 0 else lax.rem(places[a] + d, counts[a])

    def block_of(a, d):
        return pl.ds(place_of(a, d) * sizes[a], sizes[a])

    remote = [(a, d) for d in range(1, most) for a in range(2) if d < counts[a]]

    def chunk(m):
        if isinstance(m, int) and m < len(EARLY):
            below, size = EARLY[m]
            return pl.ds(sky_rows - below, size)
        start = sky_rows - BLOCK - STEP * (m - len(EARLY) + 1)
        return pl.ds(pl.multiple_of(start, STEP), STEP)

    def swap(view, sem):
        return pltpu.make_async_remote_copy(
            give.at[view], take.at[view], send_sem.at[0], swap_sem.at[sem],
            device_id={"pgroup": partner}, device_id_type=MESH,
        )

    def swap_part(m, n):
        a, d = remote[n]
        return swap((a, block_of(a, d), chunk(m)), m * len(remote) + n)

    def swap_home(a):
        rows = pl.ds(sky_rows - BLOCK, BLOCK)
        return swap((a, block_of(a, 0), rows), FINE * len(remote) + a)

    def swap_all(m):
        return swap((slice(None), slice(None), chunk(m)), FINE * len(remote) + 2 + m - FINE)

    def first_copy(m, a, d):
        rows = chunk(m)
        at = pl.ds(offsets[a] + (d - 1) * sizes[a], sizes[a])
        return pltpu.make_async_remote_copy(
            canvas.at[a, block_of(a, d), rows], inbox.at[at, rows],
            send_sem.at[1], first_sem.at[m],
            device_id={"pgroup": peers[a][d - 1]}, device_id_type=MESH,
        )

    def second_copy(m, a, d):
        rows = chunk(m)
        source = place_of(a, 0) * sizes[a] + place_of(1 - a, d) * half
        at = pl.ds(second_tiles[a] + (d - 1) * half, half)
        return pltpu.make_async_remote_copy(
            canvas.at[a, pl.ds(source, half), rows], inbox.at[at, rows],
            send_sem.at[1], second_sem.at[m],
            device_id={"pgroup": peers[1 - a][d - 1]}, device_id_type=MESH,
        )

    def arrived(view, sem):
        pltpu.make_async_copy(view, view, sem).wait()

    def put(target, a, slot, sky_tile, rows, start, terms, index, above, index_above, last, extra):
        total = sum_rows(a, terms, index, start, rows.size)
        if extra is not None:
            total = total + extra[a, slot, rows]
        target[a, slot, rows] = total
        if start == 0:
            top = total[:8] + sum_rows(a, above, index_above, BLOCK, 8)
            if last:
                top = top + halo_in[a, sky_tile]
            target[a, slot, pl.ds(rows.start, 8)] = top

    def cover(target, which, rows, sky_block, start, arrays, chips, last, extra):
        terms = block_terms(sky_block)
        above = block_terms(sky_block - 1) if start == 0 else None

        def one(n, _):
            chip_at = chips(n)
            for q in range(half):
                sky_tile = chip_at * own + which * half + q
                index = indices(terms, sky_tile)
                index_above = indices(above, sky_tile) if start == 0 else None
                for a in arrays:
                    put(
                        target, a, slot_of(a, chip_at) + q, sky_tile, rows, start,
                        terms, index, above, index_above, last, extra,
                    )
            return 0

        return one

    def part(target, which, rows, start, a, d, extra):
        at = place_of(a, d)
        chips = (lambda n: n * nx + at) if a == 0 else (lambda n: at * nx + n)
        one = cover(target, which, rows, TILE_BLOCKS - 1, start, (a,), chips, False, extra)
        lax.fori_loop(0, counts[1 - a], one, 0)

    def begin(m):
        for n, (a, d) in enumerate(remote):
            part(give, 1 - core, chunk(m), BLOCK - EARLY[m][0], a, d, None)
            swap_part(m, n).start()

    def release(m):
        for n, (a, d) in enumerate(remote):
            swap_part(m, n).wait_recv()
            part(canvas, core, chunk(m), BLOCK - EARLY[m][0], a, d, take)
            first_copy(m, a, d).start()

    def home(target, which, extra):
        for a in range(2):
            if extra is not None:
                swap_home(a).wait_recv()
            for start in range(0, BLOCK, STEP):
                part(target, which, pl.ds(sky_rows - BLOCK + start, STEP), start, a, 0, extra)
            if extra is None:
                swap_home(a).start()

    def build(m, sky_block, start, last=False):
        one = cover(give, 1 - core, chunk(m), sky_block, start, (0, 1), lambda n: n, last, None)
        lax.fori_loop(0, ny * nx, one, 0)
        swap_all(m).start()

    def combine(m, sky_block, start, last=False):
        swap_all(m).wait_recv()
        one = cover(canvas, core, chunk(m), sky_block, start, (0, 1), lambda n: n, last, take)
        lax.fori_loop(0, ny * nx, one, 0)
        for a, d in remote:
            first_copy(m, a, d).start()

    halo = pltpu.make_async_remote_copy(
        halo_out, halo_in, halo_sem.at[0], halo_sem.at[1],
        device_id={"tile": after}, device_id_type=MESH,
    )

    top = TILE_BLOCKS - 1
    top_terms = block_terms(top)

    def border(sky_tile, _):
        index = indices(top_terms, sky_tile)
        for a in range(2):
            halo_out[a, sky_tile] = sum_rows(a, top_terms, index, BLOCK, 8)
        return 0

    bottom = blocks - 1
    loaded(0)
    interpolate(bottom, 104, 128, 3)
    pl.semaphore_wait(barrier, len(near) + jnp.where(tile > 0, 1, 0))
    begin(0)

    @pl.when(tile > 0)
    def _():
        pl.semaphore_signal(entered, inc=1, device_id={"tile": before}, device_id_type=MESH)

    @pl.when(tile == 0)
    def _():
        halo_in[...] = jnp.zeros(halo_in.shape, F32)

    loaded(1)
    interpolate(bottom, 88, 104, 2)
    begin(1)
    release(0)
    loaded(2)
    interpolate(bottom, 56, 88, 4)
    release(1)
    begin(2)
    interpolate(bottom, 0, 56, 7)
    release(2)
    for k, b in enumerate(reversed(range(blocks - 1))):
        loaded(len(PIECES) + k)
        interpolate(b, 112, 128, 2)
    begin(3)
    for b in reversed(range(blocks - 1)):
        interpolate(b, 40, 112, 3)
    release(3)
    for b in reversed(range(blocks - 1)):
        interpolate(b, 0, 40, 5)
    build(FINE, top - 1, STEP)
    home(give, 1 - core, None)
    lax.fori_loop(0, sky_tiles, border, 0, unroll=4)

    @pl.when(tile < n_tile - 1)
    def _():
        pl.semaphore_wait(entered, 1)
        halo.start()

    def spread(i, _):
        at = top - 1 - i
        build(FINE + 1 + 2 * i, at, 0)
        combine(FINE + 2 * i, at, STEP)
        build(FINE + 2 + 2 * i, at - 1, STEP)
        combine(FINE + 1 + 2 * i, at, 0)
        return 0

    lax.fori_loop(0, top - 1, spread, 0)

    @pl.when(tile > 0)
    def _():
        halo.wait_recv()

    build(chunks - 1, 0, 0, last=True)
    combine(chunks - 2, 0, STEP)
    combine(chunks - 1, 0, 0, last=True)
    home(canvas, core, take)

    def every(step):
        for m in range(len(EARLY)):
            step(m)

        def one(m, _):
            step(m)
            return 0

        lax.fori_loop(len(EARLY), chunks, one, 0)

    def middle(m):
        rows = chunk(m)
        arrived(inbox.at[pl.ds(0, first_tiles), rows], first_sem.at[m])
        for a in range(2):
            for e in range(1, counts[1 - a]):
                at = place_of(1 - a, e) * half

                def one(q, _):
                    slot = place_of(a, 0) * sizes[a] + at + q
                    total = canvas[a, slot, rows]
                    for d in range(counts[a] - 1):
                        total = total + inbox[offsets[a] + d * sizes[a] + at + q, rows]
                    canvas[a, slot, rows] = total
                    return 0

                lax.fori_loop(0, half, one, 0, unroll=True)
                second_copy(m, a, e).start()

    every(middle)

    def finish(m):
        rows = chunk(m)
        arrived(inbox.at[pl.ds(first_tiles, every_tile - first_tiles), rows], second_sem.at[m])
        for q in range(half):
            sums = []
            for a in range(2):
                at = places[1 - a] * half + q
                total = canvas[a, place_of(a, 0) * sizes[a] + at, rows]
                for d in range(counts[a] - 1):
                    total = total + inbox[offsets[a] + d * sizes[a] + at, rows]
                for e in range(counts[1 - a] - 1):
                    total = total + inbox[second_tiles[a] + e * half + q, rows]
                sums.append(total)
            lanes = slice(q * LANES, (q + 1) * LANES)
            numer[rows, lanes] = sums[0]
            weight[rows, lanes] = sums[1]
            normalised[rows, lanes] = sums[0] / jnp.maximum(sums[1], 0.05)

    every(finish)
    arrived(give, send_sem.at[0])
    arrived(inbox, send_sem.at[1])

    @pl.when(tile < n_tile - 1)
    def _():
        halo.wait_send()


def copy_out(numer, weight, normalised, numer_out, weight_out, normalised_out, sem):
    pairs = ((numer, numer_out), (weight, weight_out), (normalised, normalised_out))
    copies = [pltpu.make_async_copy(a, b, sem.at[n]) for n, (a, b) in enumerate(pairs)]
    for copy in copies:
        copy.start()
    for copy in copies:
        copy.wait()


def body(ny, nx, n_tile, images, beams, row_block, col_block, band, row_frac, col_frac):
    points, img_rows, width = images.shape
    blocks = img_rows // BLOCK
    col_tiles = width // LANES
    sky_tiles = SKY_COLS // LANES
    sky_rows = TILE_BLOCKS * BLOCK
    half = sky_tiles // (2 * ny * nx)
    per_core = sky_tiles // 2
    chunks = len(EARLY) + (TILE_BLOCKS - 1) * (BLOCK // STEP)
    own_cols = half * LANES
    inbox_tiles = (nx - 1) * (ny + 1) * half + (ny - 1) * (nx + 1) * half
    dma = pltpu.SemaphoreType.DMA
    anywhere = pl.BlockSpec(memory_space=pl.ANY)
    scalars = [pltpu.SMEM(v.shape, v.dtype) for v in (row_block, col_block, band, row_frac, col_frac)]
    vmem = pl.BlockSpec(memory_space=pltpu.VMEM)
    out = pltpu.VMEM((sky_rows, own_cols), F32)
    numer, weight, normalised = pl.pallas_call(
        functools.partial(kernel, ny, nx, n_tile),
        out_shape=(out, out, out),
        in_specs=[anywhere] * 7,
        out_specs=(vmem, vmem, vmem),
        scratch_shapes=scalars + [
            pltpu.VMEM((2, points, img_rows, width), F32),
            pltpu.VMEM((2, points * blocks * col_tiles + 1, BLOCK + 2 * PAD, LANES), F32),
            pltpu.VMEM((2, sky_tiles, 8, LANES), F32),
            pltpu.VMEM((2, sky_tiles, 8, LANES), F32),
            pltpu.VMEM((2, per_core, sky_rows, LANES), F32),
            pltpu.VMEM((2, per_core, sky_rows, LANES), F32),
            pltpu.VMEM((2, per_core, sky_rows, LANES), F32),
            pltpu.VMEM((inbox_tiles, sky_rows, LANES), F32),
            dma((5,)),
            dma((len(PIECES) + blocks - 1,)),
            dma((2,)),
            pltpu.SemaphoreType.REGULAR,
            dma((FINE * (nx + ny - 2) + 2 + chunks - FINE,)),
            dma((chunks,)),
            dma((chunks,)),
            dma((2,)),
        ],
        compiler_params=pltpu.CompilerParams(
            collective_id=0, has_side_effects=True, vmem_limit_bytes=56 * 1024 * 1024
        ),
        name="combine",
    )(images, beams, row_block, col_block, band, row_frac, col_frac)
    flat = jax.ShapeDtypeStruct((sky_rows, own_cols), F32)
    return pl.pallas_call(
        copy_out,
        out_shape=(flat, flat, flat),
        in_specs=[vmem] * 3,
        out_specs=(anywhere,) * 3,
        scratch_shapes=[dma((3,))],
        name="copy_out",
    )(*[pltpu.with_memory_space_constraint(v, pltpu.VMEM) for v in (numer, weight, normalised)])


def solution(mesh):
    ny, nx = chip_grid(mesh.shape["pgroup"])
    return jax.shard_map(
        functools.partial(body, ny, nx, mesh.shape["tile"]),
        mesh=mesh,
        in_specs=(
            P(("pgroup", "tile"), None, None),
            P(("pgroup", "tile"), None, None),
            P(("pgroup", "tile")),
            P(("pgroup", "tile")),
            P(("pgroup", "tile"), None),
            P(("pgroup", "tile")),
            P(("pgroup", "tile")),
        ),
        out_specs=(P("tile", "pgroup"), P("tile", "pgroup"), P("tile", "pgroup")),
        check_vma=False,
    )
```

```python
import functools
import math

import jax
import jax.numpy as jnp
from jax import lax
from jax.experimental import pallas as pl
from jax.experimental.pallas import tpu as pltpu
from jax.sharding import PartitionSpec as P

TILE_BLOCKS = 4
SKY_COLS = 4096
LANES = 128
BLOCK = 128
PAD = 8
STEP = 64
START = 32
READY = START + PAD
PIECES = ((104, 128), (80, 104), (0, 80))
EARLY = ((16, 16), (40, 24), (64, 24), (BLOCK, STEP))
FINE = len(EARLY)
DETOUR = 1
MESH = pl.DeviceIdType.MESH
F32 = jnp.float32


def chip_grid(groups):
    chips = groups // 2
    along_x = math.isqrt(chips)
    while chips % along_x:
        along_x -= 1
    return chips // along_x, along_x


def kernel(
    ny, nx, n_tile,
    images, beams, row_block_in, col_block_in, band_in, row_frac_in, col_frac_in,
    numer, weight, normalised,
    row_block, col_block, band, row_frac, col_frac,
    raw, shaped, halo_out, halo_in, give, take, canvas,
    inbox, detour,
    small_sem, load_sem, halo_sem, entered, swap_sem, first_sem, second_sem, send_sem, detour_sem,
):
    points, img_rows, width = images.shape
    blocks = img_rows // BLOCK
    col_tiles = width // LANES
    sky_tiles = SKY_COLS // LANES
    sky_rows = TILE_BLOCKS * BLOCK
    own = sky_tiles // (ny * nx)
    half = own // 2
    per_core = sky_tiles // 2
    empty = points * blocks * col_tiles
    chunks = len(EARLY) + (TILE_BLOCKS - 1) * (BLOCK // STEP)

    me = lax.axis_index("pgroup")
    tile = lax.axis_index("tile")
    core = lax.rem(me, 2)
    chip = me // 2
    x = lax.rem(chip, nx)
    y = chip // nx
    partner = me + 1 - 2 * core
    x_peers = [(y * nx + lax.rem(x + d, nx)) * 2 + core for d in range(1, nx)]
    y_peers = [(lax.rem(y + d, ny) * nx + x) * 2 + core for d in range(1, ny)]
    counts = (nx, ny)
    most = max(nx, ny)
    places = (x, y)
    peers = (x_peers, y_peers)
    sizes = (per_core // nx, per_core // ny)
    offsets = (0, (nx - 1) * sizes[0])
    first_tiles = offsets[1] + (ny - 1) * sizes[1]
    second_tiles = (first_tiles, first_tiles + (ny - 1) * half)
    every_tile = second_tiles[1] + (nx - 1) * half
    after = lax.rem(tile + 1, n_tile)
    before = lax.rem(tile + n_tile - 1, n_tile)

    pieces = [(img_rows - BLOCK + low, high - low) for low, high in PIECES]
    pieces += [(b * BLOCK, BLOCK) for b in reversed(range(blocks - 1))]

    def load(k):
        low, size = pieces[k]
        for p in range(points):
            for which, source in enumerate((images, beams)):
                rows = pl.ds(low, size)
                pltpu.make_async_copy(
                    source.at[p, rows], raw.at[which, p, rows], load_sem.at[k]
                ).start()

    load(0)
    small = [
        pltpu.make_async_copy(source, target, small_sem.at[n])
        for n, (source, target) in enumerate((
            (row_block_in, row_block), (col_block_in, col_block), (band_in, band),
            (row_frac_in, row_frac), (col_frac_in, col_frac),
        ))
    ]
    for copy in small:
        copy.start()
    for k in range(1, len(pieces)):
        load(k)

    barrier = pltpu.get_barrier_semaphore()
    near = [partner] + x_peers + y_peers
    for q in near:
        pl.semaphore_signal(barrier, inc=1, device_id={"pgroup": q}, device_id_type=MESH)

    @pl.when(tile < n_tile - 1)
    def _():
        pl.semaphore_signal(barrier, inc=1, device_id={"tile": after}, device_id_type=MESH)

    def clear(index, _):
        for a in range(2):
            shaped[a, index, :PAD] = jnp.zeros((PAD, LANES), F32)
            shaped[a, index, PAD + BLOCK :] = jnp.zeros((PAD, LANES), F32)
        return 0

    lax.fori_loop(0, empty, clear, 0, unroll=8)
    for a in range(2):
        shaped[a, empty] = jnp.zeros((BLOCK + 2 * PAD, LANES), F32)
    for copy in small:
        copy.wait()

    first_lane = lax.broadcasted_iota(jnp.int32, (8, LANES), 1) == 0
    across = [(1.0 - col_frac[p], col_frac[p]) for p in range(points)]
    down = [(1.0 - row_frac[p], row_frac[p]) for p in range(points)]
    base_block = [row_block[p] - tile * TILE_BLOCKS for p in range(points)]
    base_tile = [col_block[p] for p in range(points)]

    def loaded(k):
        low, size = pieces[k]
        view = raw.at[:, :, pl.ds(low, size)]
        pltpu.make_async_copy(view, view, load_sem.at[k]).wait()

    def interpolate(b, low, high, unroll):
        def one(r, _):
            source = pl.ds(pl.multiple_of(b * BLOCK + 8 * r, 8), 8)
            target = pl.ds(pl.multiple_of(PAD + 8 * r, 8), 8)
            for p in range(points):
                stay, go = across[p]
                prior = [jnp.zeros((8, LANES), F32)] * 2
                for t in range(col_tiles):
                    lanes = slice(t * LANES, (t + 1) * LANES)
                    beam = raw[1, p, source, lanes]
                    image = raw[0, p, source, lanes]
                    for a, here in enumerate((beam * image, beam * beam)):
                        turned = pltpu.roll(here, 1, 1)
                        moved = jnp.where(first_lane, prior[a], turned)
                        shaped[a, (p * blocks + b) * col_tiles + t, target] = stay * here + go * moved
                        prior[a] = turned
            return 0

        lax.fori_loop(low // 8, high // 8, one, 0, unroll=unroll)

    def block_terms(sky_block):
        terms = []
        for p in range(points):
            b = sky_block - base_block[p]
            within = (b >= 0) & (b < blocks)
            b = jnp.clip(b, 0, blocks - 1)
            shift = band[p, b]
            at = jnp.where(within, base_tile[p], sky_tiles)
            terms.append((at, (p * blocks + b) * col_tiles - base_tile[p], PAD - shift))
        return terms

    def indices(terms, sky_tile):
        found = []
        for at, base, _ in terms:
            t = sky_tile - at
            found.append(jnp.where((t >= 0) & (t < col_tiles), base + sky_tile, empty))
        return found

    def sum_rows(a, terms, index, start, size):
        total = None
        for p in range(points):
            at = terms[p][2] + start
            low = shaped[a, index[p], pl.ds(at, size)]
            high = shaped[a, index[p], pl.ds(at - 1, size)]
            term = down[p][0] * low + down[p][1] * high
            total = term if total is None else total + term
        return total

    def slot_of(a, chip_at):
        if a == 1:
            return chip_at * half
        return (lax.rem(chip_at, nx) * ny + chip_at // nx) * half

    def place_of(a, d):
        return places[a] if d == 0 else lax.rem(places[a] + d, counts[a])

    def block_of(a, d):
        return pl.ds(place_of(a, d) * sizes[a], sizes[a])

    remote = [(a, d) for d in range(1, most) for a in range(2) if d < counts[a]]

    def chunk(m):
        if isinstance(m, int) and m < len(EARLY):
            below, size = EARLY[m]
            return pl.ds(sky_rows - below, size)
        start = sky_rows - BLOCK - STEP * (m - len(EARLY) + 1)
        return pl.ds(pl.multiple_of(start, STEP), STEP)

    def swap(view, sem):
        return pltpu.make_async_remote_copy(
            give.at[view], take.at[view], send_sem.at[0], swap_sem.at[sem],
            device_id={"pgroup": partner}, device_id_type=MESH,
        )

    def swap_part(m, n):
        a, d = remote[n]
        return swap((a, block_of(a, d), chunk(m)), m * len(remote) + n)

    def swap_home(a):
        rows = pl.ds(sky_rows - BLOCK, BLOCK)
        return swap((a, block_of(a, 0), rows), FINE * len(remote) + a)

    def swap_all(m):
        return swap((slice(None), slice(None), chunk(m)), FINE * len(remote) + 2 + m - FINE)

    def first_copy(m, a, d):
        rows = chunk(m)
        at = pl.ds(offsets[a] + (d - 1) * sizes[a], sizes[a])
        return pltpu.make_async_remote_copy(
            canvas.at[a, block_of(a, d), rows], inbox.at[at, rows],
            send_sem.at[1], first_sem.at[m],
            device_id={"pgroup": peers[a][d - 1]}, device_id_type=MESH,
        )

    def second_copy(m, a, d):
        rows = chunk(m)
        source = place_of(a, 0) * sizes[a] + place_of(1 - a, d) * half
        at = pl.ds(second_tiles[a] + (d - 1) * half, half)
        return pltpu.make_async_remote_copy(
            canvas.at[a, pl.ds(source, half), rows], inbox.at[at, rows],
            send_sem.at[1], second_sem.at[m],
            device_id={"pgroup": peers[1 - a][d - 1]}, device_id_type=MESH,
        )

    square = nx == 2 and ny == 2

    def at_corner(a, first, second):
        return (places[a] == first) & (places[1 - a] == second)

    def short_copy(a):
        rows = chunk(DETOUR)
        return pltpu.make_async_remote_copy(
            canvas.at[a, pl.ds(0, half), rows], inbox.at[pl.ds(offsets[a], half), rows],
            send_sem.at[1], first_sem.at[DETOUR],
            device_id={"pgroup": peers[a][0]}, device_id_type=MESH,
        )

    def detour_copy(a):
        return pltpu.make_async_remote_copy(
            canvas.at[a, pl.ds(half, half), chunk(DETOUR)], detour.at[a],
            send_sem.at[1], detour_sem.at[a],
            device_id={"pgroup": peers[1 - a][0]}, device_id_type=MESH,
        )

    def late_copy(a):
        rows = chunk(DETOUR)
        return pltpu.make_async_remote_copy(
            canvas.at[a, pl.ds(half, half), rows], inbox.at[pl.ds(offsets[a] + half, half), rows],
            send_sem.at[1], second_sem.at[DETOUR],
            device_id={"pgroup": peers[a][0]}, device_id_type=MESH,
        )

    def send_first(m, a, d):
        if not (square and isinstance(m, int) and m == DETOUR):
            first_copy(m, a, d).start()
            return

        @pl.when(places[a] == 0)
        def _():
            first_copy(m, a, d).start()

        @pl.when(places[a] == 1)
        def _():
            short_copy(a).start()

        @pl.when(at_corner(a, 1, 0))
        def _():
            detour_copy(a).start()

    def arrived(view, sem):
        pltpu.make_async_copy(view, view, sem).wait()

    def put(target, a, slot, sky_tile, rows, start, terms, index, above, index_above, last, extra):
        total = sum_rows(a, terms, index, start, rows.size)
        if extra is not None:
            total = total + extra[a, slot, rows]
        target[a, slot, rows] = total
        if start == 0:
            top = total[:8] + sum_rows(a, above, index_above, BLOCK, 8)
            if last:
                top = top + halo_in[a, sky_tile]
            target[a, slot, pl.ds(rows.start, 8)] = top

    def cover(target, which, rows, sky_block, start, arrays, chips, last, extra):
        terms = block_terms(sky_block)
        above = block_terms(sky_block - 1) if start == 0 else None

        def one(n, _):
            chip_at = chips(n)
            for q in range(half):
                sky_tile = chip_at * own + which * half + q
                index = indices(terms, sky_tile)
                index_above = indices(above, sky_tile) if start == 0 else None
                for a in arrays:
                    put(
                        target, a, slot_of(a, chip_at) + q, sky_tile, rows, start,
                        terms, index, above, index_above, last, extra,
                    )
            return 0

        return one

    def part(target, which, rows, start, a, d, extra):
        at = place_of(a, d)
        chips = (lambda n: n * nx + at) if a == 0 else (lambda n: at * nx + n)
        one = cover(target, which, rows, TILE_BLOCKS - 1, start, (a,), chips, False, extra)
        lax.fori_loop(0, counts[1 - a], one, 0)

    def begin(m):
        for n, (a, d) in enumerate(remote):
            part(give, 1 - core, chunk(m), BLOCK - EARLY[m][0], a, d, None)
            swap_part(m, n).start()

    def release(m):
        for n, (a, d) in enumerate(remote):
            swap_part(m, n).wait_recv()
            part(canvas, core, chunk(m), BLOCK - EARLY[m][0], a, d, take)
            send_first(m, a, d)

    def home(target, which, extra):
        for a in range(2):
            if extra is not None:
                swap_home(a).wait_recv()
            for start in range(0, BLOCK, STEP):
                part(target, which, pl.ds(sky_rows - BLOCK + start, STEP), start, a, 0, extra)
            if extra is None:
                swap_home(a).start()

    def build(m, sky_block, start, last=False):
        one = cover(give, 1 - core, chunk(m), sky_block, start, (0, 1), lambda n: n, last, None)
        lax.fori_loop(0, ny * nx, one, 0)
        swap_all(m).start()

    def combine(m, sky_block, start, last=False):
        swap_all(m).wait_recv()
        one = cover(canvas, core, chunk(m), sky_block, start, (0, 1), lambda n: n, last, take)
        lax.fori_loop(0, ny * nx, one, 0)
        for a, d in remote:
            first_copy(m, a, d).start()

    halo = pltpu.make_async_remote_copy(
        halo_out, halo_in, halo_sem.at[0], halo_sem.at[1],
        device_id={"tile": after}, device_id_type=MESH,
    )

    top = TILE_BLOCKS - 1
    top_terms = block_terms(top)

    def border(sky_tile, _):
        index = indices(top_terms, sky_tile)
        for a in range(2):
            halo_out[a, sky_tile] = sum_rows(a, top_terms, index, BLOCK, 8)
        return 0

    bottom = blocks - 1
    loaded(0)
    interpolate(bottom, 104, 128, 3)
    pl.semaphore_wait(barrier, len(near) + jnp.where(tile > 0, 1, 0))
    begin(0)

    @pl.when(tile > 0)
    def _():
        pl.semaphore_signal(entered, inc=1, device_id={"tile": before}, device_id_type=MESH)

    @pl.when(tile == 0)
    def _():
        halo_in[...] = jnp.zeros(halo_in.shape, F32)

    loaded(1)
    interpolate(bottom, 80, 104, 3)
    begin(1)
    release(0)
    loaded(2)
    interpolate(bottom, 56, 80, 3)
    release(1)
    begin(2)
    interpolate(bottom, 0, 56, 7)
    release(2)
    for k, b in enumerate(reversed(range(blocks - 1))):
        loaded(len(PIECES) + k)
        interpolate(b, 112, 128, 2)
    begin(3)
    for b in reversed(range(blocks - 1)):
        interpolate(b, 40, 112, 3)
    release(3)
    for b in reversed(range(blocks - 1)):
        interpolate(b, 0, 40, 5)
    build(FINE, top - 1, STEP)
    home(give, 1 - core, None)
    lax.fori_loop(0, sky_tiles, border, 0, unroll=4)

    @pl.when(tile < n_tile - 1)
    def _():
        pl.semaphore_wait(entered, 1)
        halo.start()

    def spread(i, _):
        at = top - 1 - i
        build(FINE + 1 + 2 * i, at, 0)
        combine(FINE + 2 * i, at, STEP)
        build(FINE + 2 + 2 * i, at - 1, STEP)
        combine(FINE + 1 + 2 * i, at, 0)
        return 0

    lax.fori_loop(0, top - 1, spread, 0)

    @pl.when(tile > 0)
    def _():
        halo.wait_recv()

    build(chunks - 1, 0, 0, last=True)
    combine(chunks - 2, 0, STEP)
    combine(chunks - 1, 0, 0, last=True)
    home(canvas, core, take)

    def every(step):
        for m in range(len(EARLY)):
            step(m)

        def one(m, _):
            step(m)
            return 0

        lax.fori_loop(len(EARLY), chunks, one, 0)

    def middle(m):
        rows = chunk(m)
        bent = square and isinstance(m, int) and m == DETOUR
        if bent:
            for n in range(3):
                @pl.when(x + y == n)
                def _():
                    arrived(inbox.at[pl.ds(0, (2 + n) * half), rows], first_sem.at[m])
        else:
            arrived(inbox.at[pl.ds(0, first_tiles), rows], first_sem.at[m])
        for a in range(2):
            for e in range(1, counts[1 - a]):
                at = place_of(1 - a, e) * half

                def one(q, _):
                    slot = place_of(a, 0) * sizes[a] + at + q
                    total = canvas[a, slot, rows]
                    for d in range(counts[a] - 1):
                        total = total + inbox[offsets[a] + d * sizes[a] + at + q, rows]
                    canvas[a, slot, rows] = total
                    return 0

                if bent:
                    @pl.when(~at_corner(a, 0, 0))
                    def _():
                        lax.fori_loop(0, half, one, 0, unroll=True)
                else:
                    lax.fori_loop(0, half, one, 0, unroll=True)
                second_copy(m, a, e).start()
            if bent:
                @pl.when(at_corner(a, 1, 1))
                def _():
                    arrived(detour.at[a], detour_sem.at[a])
                    for q in range(half):
                        canvas[a, half + q, rows] += detour[a, q]
                    late_copy(a).start()

    every(middle)

    def finish(m):
        rows = chunk(m)
        second_count = every_tile - first_tiles
        if square and isinstance(m, int) and m == DETOUR:
            @pl.when(x == y)
            def _():
                arrived(inbox.at[pl.ds(0, second_count), rows], second_sem.at[m])

            @pl.when(x != y)
            def _():
                arrived(inbox.at[pl.ds(0, second_count + half), rows], second_sem.at[m])
        else:
            arrived(inbox.at[pl.ds(first_tiles, second_count), rows], second_sem.at[m])
        for q in range(half):
            sums = []
            for a in range(2):
                at = places[1 - a] * half + q
                total = canvas[a, place_of(a, 0) * sizes[a] + at, rows]
                for d in range(counts[a] - 1):
                    total = total + inbox[offsets[a] + d * sizes[a] + at, rows]
                for e in range(counts[1 - a] - 1):
                    total = total + inbox[second_tiles[a] + e * half + q, rows]
                sums.append(total)
            lanes = slice(q * LANES, (q + 1) * LANES)
            numer[rows, lanes] = sums[0]
            weight[rows, lanes] = sums[1]
            normalised[rows, lanes] = sums[0] / jnp.maximum(sums[1], 0.05)

    every(finish)
    arrived(give, send_sem.at[0])
    arrived(inbox, send_sem.at[1])

    @pl.when(tile < n_tile - 1)
    def _():
        halo.wait_send()


def copy_out(numer, weight, normalised, numer_out, weight_out, normalised_out, sem):
    pairs = ((numer, numer_out), (weight, weight_out), (normalised, normalised_out))
    copies = [pltpu.make_async_copy(a, b, sem.at[n]) for n, (a, b) in enumerate(pairs)]
    for copy in copies:
        copy.start()
    for copy in copies:
        copy.wait()


def body(ny, nx, n_tile, images, beams, row_block, col_block, band, row_frac, col_frac):
    points, img_rows, width = images.shape
    blocks = img_rows // BLOCK
    col_tiles = width // LANES
    sky_tiles = SKY_COLS // LANES
    sky_rows = TILE_BLOCKS * BLOCK
    half = sky_tiles // (2 * ny * nx)
    per_core = sky_tiles // 2
    chunks = len(EARLY) + (TILE_BLOCKS - 1) * (BLOCK // STEP)
    own_cols = half * LANES
    inbox_tiles = (nx - 1) * (ny + 1) * half + (ny - 1) * (nx + 1) * half
    dma = pltpu.SemaphoreType.DMA
    anywhere = pl.BlockSpec(memory_space=pl.ANY)
    scalars = [pltpu.SMEM(v.shape, v.dtype) for v in (row_block, col_block, band, row_frac, col_frac)]
    vmem = pl.BlockSpec(memory_space=pltpu.VMEM)
    out = pltpu.VMEM((sky_rows, own_cols), F32)
    numer, weight, normalised = pl.pallas_call(
        functools.partial(kernel, ny, nx, n_tile),
        out_shape=(out, out, out),
        in_specs=[anywhere] * 7,
        out_specs=(vmem, vmem, vmem),
        scratch_shapes=scalars + [
            pltpu.VMEM((2, points, img_rows, width), F32),
            pltpu.VMEM((2, points * blocks * col_tiles + 1, BLOCK + 2 * PAD, LANES), F32),
            pltpu.VMEM((2, sky_tiles, 8, LANES), F32),
            pltpu.VMEM((2, sky_tiles, 8, LANES), F32),
            pltpu.VMEM((2, per_core, sky_rows, LANES), F32),
            pltpu.VMEM((2, per_core, sky_rows, LANES), F32),
            pltpu.VMEM((2, per_core, sky_rows, LANES), F32),
            pltpu.VMEM((inbox_tiles, sky_rows, LANES), F32),
            pltpu.VMEM((2, half, EARLY[DETOUR][1], LANES), F32),
            dma((5,)),
            dma((len(PIECES) + blocks - 1,)),
            dma((2,)),
            pltpu.SemaphoreType.REGULAR,
            dma((FINE * (nx + ny - 2) + 2 + chunks - FINE,)),
            dma((chunks,)),
            dma((chunks,)),
            dma((2,)),
            dma((2,)),
        ],
        compiler_params=pltpu.CompilerParams(
            collective_id=0, has_side_effects=True, vmem_limit_bytes=56 * 1024 * 1024
        ),
        name="combine",
    )(images, beams, row_block, col_block, band, row_frac, col_frac)
    flat = jax.ShapeDtypeStruct((sky_rows, own_cols), F32)
    return pl.pallas_call(
        copy_out,
        out_shape=(flat, flat, flat),
        in_specs=[vmem] * 3,
        out_specs=(anywhere,) * 3,
        scratch_shapes=[dma((3,))],
        name="copy_out",
    )(*[pltpu.with_memory_space_constraint(v, pltpu.VMEM) for v in (numer, weight, normalised)])


def solution(mesh):
    ny, nx = chip_grid(mesh.shape["pgroup"])
    return jax.shard_map(
        functools.partial(body, ny, nx, mesh.shape["tile"]),
        mesh=mesh,
        in_specs=(
            P(("pgroup", "tile"), None, None),
            P(("pgroup", "tile"), None, None),
            P(("pgroup", "tile")),
            P(("pgroup", "tile")),
            P(("pgroup", "tile"), None),
            P(("pgroup", "tile")),
            P(("pgroup", "tile")),
        ),
        out_specs=(P("tile", "pgroup"), P("tile", "pgroup"), P("tile", "pgroup")),
        check_vma=False,
    )
```

```python
import functools
import math

import jax
import jax.numpy as jnp
from jax import lax
from jax.experimental import pallas as pl
from jax.experimental.pallas import tpu as pltpu
from jax.sharding import PartitionSpec as P

TILE_BLOCKS = 4
SKY_COLS = 4096
LANES = 128
BLOCK = 128
PAD = 8
STEP = 64
START = 32
READY = START + PAD
PIECES = ((104, 128), (80, 104), (0, 80))
EARLY = ((16, 16), (40, 24), (64, 24), (BLOCK, STEP))
FINE = len(EARLY)
DETOUR = 1
GROUPS = ((0, 2, 3), (DETOUR,), (4, 5), (6, 7), (8,), (9,))
MESH = pl.DeviceIdType.MESH
F32 = jnp.float32


def chip_grid(groups):
    chips = groups // 2
    along_x = math.isqrt(chips)
    while chips % along_x:
        along_x -= 1
    return chips // along_x, along_x


def kernel(
    ny, nx, n_tile,
    images, beams, row_block_in, col_block_in, band_in, row_frac_in, col_frac_in,
    numer, weight, normalised,
    row_block, col_block, band, row_frac, col_frac,
    raw, shaped, halo_out, halo_in, give, take, canvas,
    inbox, detour,
    small_sem, load_sem, halo_sem, entered, swap_sem, first_sem, second_sem, send_sem, detour_sem,
):
    points, img_rows, width = images.shape
    blocks = img_rows // BLOCK
    col_tiles = width // LANES
    sky_tiles = SKY_COLS // LANES
    sky_rows = TILE_BLOCKS * BLOCK
    own = sky_tiles // (ny * nx)
    half = own // 2
    per_core = sky_tiles // 2
    empty = points * blocks * col_tiles
    chunks = len(EARLY) + (TILE_BLOCKS - 1) * (BLOCK // STEP)

    me = lax.axis_index("pgroup")
    tile = lax.axis_index("tile")
    core = lax.rem(me, 2)
    chip = me // 2
    x = lax.rem(chip, nx)
    y = chip // nx
    partner = me + 1 - 2 * core
    x_peers = [(y * nx + lax.rem(x + d, nx)) * 2 + core for d in range(1, nx)]
    y_peers = [(lax.rem(y + d, ny) * nx + x) * 2 + core for d in range(1, ny)]
    counts = (nx, ny)
    most = max(nx, ny)
    places = (x, y)
    peers = (x_peers, y_peers)
    sizes = (per_core // nx, per_core // ny)
    offsets = (0, (nx - 1) * sizes[0])
    first_tiles = offsets[1] + (ny - 1) * sizes[1]
    second_tiles = (first_tiles, first_tiles + (ny - 1) * half)
    every_tile = second_tiles[1] + (nx - 1) * half
    after = lax.rem(tile + 1, n_tile)
    before = lax.rem(tile + n_tile - 1, n_tile)

    pieces = [(img_rows - BLOCK + low, high - low) for low, high in PIECES]
    pieces += [(b * BLOCK, BLOCK) for b in reversed(range(blocks - 1))]

    def load(k):
        low, size = pieces[k]
        for p in range(points):
            for which, source in enumerate((images, beams)):
                step = 8 if k == 0 else size
                for at in range(low, low + size, step):
                    rows = pl.ds(at, step)
                    pltpu.make_async_copy(
                        source.at[p, rows], raw.at[which, p, rows], load_sem.at[k]
                    ).start()

    load(0)
    small = [
        pltpu.make_async_copy(source, target, small_sem.at[n])
        for n, (source, target) in enumerate((
            (row_block_in, row_block), (col_block_in, col_block), (band_in, band),
            (row_frac_in, row_frac), (col_frac_in, col_frac),
        ))
    ]
    for copy in small:
        copy.start()
    for k in range(1, len(pieces)):
        load(k)

    barrier = pltpu.get_barrier_semaphore()
    near = [partner] + x_peers + y_peers
    for q in near:
        pl.semaphore_signal(barrier, inc=1, device_id={"pgroup": q}, device_id_type=MESH)

    @pl.when(tile < n_tile - 1)
    def _():
        pl.semaphore_signal(barrier, inc=1, device_id={"tile": after}, device_id_type=MESH)

    def clear(index, _):
        for a in range(2):
            shaped[a, index, :PAD] = jnp.zeros((PAD, LANES), F32)
            shaped[a, index, PAD + BLOCK :] = jnp.zeros((PAD, LANES), F32)
        return 0

    lax.fori_loop(0, empty, clear, 0, unroll=8)
    for a in range(2):
        shaped[a, empty] = jnp.zeros((BLOCK + 2 * PAD, LANES), F32)
    for copy in small:
        copy.wait()

    first_lane = lax.broadcasted_iota(jnp.int32, (8, LANES), 1) == 0
    across = [(1.0 - col_frac[p], col_frac[p]) for p in range(points)]
    down = [(1.0 - row_frac[p], row_frac[p]) for p in range(points)]
    base_block = [row_block[p] - tile * TILE_BLOCKS for p in range(points)]
    base_tile = [col_block[p] for p in range(points)]

    def loaded(k):
        low, size = pieces[k]
        view = raw.at[:, :, pl.ds(low, size)]
        pltpu.make_async_copy(view, view, load_sem.at[k]).wait()

    def interpolate(b, low, high, unroll):
        def one(r, _):
            source = pl.ds(pl.multiple_of(b * BLOCK + 8 * r, 8), 8)
            target = pl.ds(pl.multiple_of(PAD + 8 * r, 8), 8)
            for p in range(points):
                stay, go = across[p]
                prior = [jnp.zeros((8, LANES), F32)] * 2
                for t in range(col_tiles):
                    lanes = slice(t * LANES, (t + 1) * LANES)
                    beam = raw[1, p, source, lanes]
                    image = raw[0, p, source, lanes]
                    for a, here in enumerate((beam * image, beam * beam)):
                        turned = pltpu.roll(here, 1, 1)
                        moved = jnp.where(first_lane, prior[a], turned)
                        shaped[a, (p * blocks + b) * col_tiles + t, target] = stay * here + go * moved
                        prior[a] = turned
            return 0

        lax.fori_loop(low // 8, high // 8, one, 0, unroll=unroll)

    def block_terms(sky_block):
        terms = []
        for p in range(points):
            b = sky_block - base_block[p]
            within = (b >= 0) & (b < blocks)
            b = jnp.clip(b, 0, blocks - 1)
            shift = band[p, b]
            at = jnp.where(within, base_tile[p], sky_tiles)
            terms.append((at, (p * blocks + b) * col_tiles - base_tile[p], PAD - shift))
        return terms

    def indices(terms, sky_tile):
        found = []
        for at, base, _ in terms:
            t = sky_tile - at
            found.append(jnp.where((t >= 0) & (t < col_tiles), base + sky_tile, empty))
        return found

    def sum_rows(a, terms, index, start, size):
        total = None
        for p in range(points):
            at = terms[p][2] + start
            low = shaped[a, index[p], pl.ds(at, size)]
            high = shaped[a, index[p], pl.ds(at - 1, size)]
            term = down[p][0] * low + down[p][1] * high
            total = term if total is None else total + term
        return total

    def slot_of(a, chip_at):
        if a == 1:
            return chip_at * half
        return (lax.rem(chip_at, nx) * ny + chip_at // nx) * half

    def place_of(a, d):
        return places[a] if d == 0 else lax.rem(places[a] + d, counts[a])

    def block_of(a, d):
        return pl.ds(place_of(a, d) * sizes[a], sizes[a])

    remote = [(a, d) for d in range(1, most) for a in range(2) if d < counts[a]]

    def chunk(m):
        if isinstance(m, int) and m < len(EARLY):
            below, size = EARLY[m]
            return pl.ds(sky_rows - below, size)
        start = sky_rows - BLOCK - STEP * (m - len(EARLY) + 1)
        return pl.ds(pl.multiple_of(start, STEP), STEP)

    def group_of(m):
        return [m in group for group in GROUPS].index(True)

    def group_rows(m):
        return pl.ds(0, sum(chunk(n).size for n in GROUPS[group_of(m)]))

    def opens(m):
        return GROUPS[group_of(m)][0] == m

    def swap(view, sem):
        return pltpu.make_async_remote_copy(
            give.at[view], take.at[view], send_sem.at[0], swap_sem.at[sem],
            device_id={"pgroup": partner}, device_id_type=MESH,
        )

    parts = len(remote)
    parts_tiles = sum(sizes[a] for a, _ in remote) // 2

    def swap_part(m, n):
        a, d = remote[n]
        return swap((a, block_of(a, d), chunk(m)), n if m == 0 else parts + m - 1)

    def swap_home(a):
        rows = pl.ds(sky_rows - BLOCK, BLOCK)
        return swap((a, block_of(a, 0), rows), parts + FINE - 1)

    def swap_all(m):
        return swap((slice(None), slice(None), chunk(m)), parts + m)

    def first_copy(m, a, d):
        rows = chunk(m)
        at = pl.ds(offsets[a] + (d - 1) * sizes[a], sizes[a])
        return pltpu.make_async_remote_copy(
            canvas.at[a, block_of(a, d), rows], inbox.at[at, rows],
            send_sem.at[1], first_sem.at[group_of(m)],
            device_id={"pgroup": peers[a][d - 1]}, device_id_type=MESH,
        )

    def second_copy(m, a, d):
        rows = chunk(m)
        source = place_of(a, 0) * sizes[a] + place_of(1 - a, d) * half
        at = pl.ds(second_tiles[a] + (d - 1) * half, half)
        return pltpu.make_async_remote_copy(
            canvas.at[a, pl.ds(source, half), rows], inbox.at[at, rows],
            send_sem.at[1], second_sem.at[group_of(m)],
            device_id={"pgroup": peers[1 - a][d - 1]}, device_id_type=MESH,
        )

    square = nx == 2 and ny == 2

    def at_corner(a, first, second):
        return (places[a] == first) & (places[1 - a] == second)

    def short_copy(a):
        rows = chunk(DETOUR)
        return pltpu.make_async_remote_copy(
            canvas.at[a, pl.ds(0, half), rows], inbox.at[pl.ds(offsets[a], half), rows],
            send_sem.at[1], first_sem.at[group_of(DETOUR)],
            device_id={"pgroup": peers[a][0]}, device_id_type=MESH,
        )

    def detour_copy(a):
        return pltpu.make_async_remote_copy(
            canvas.at[a, pl.ds(half, half), chunk(DETOUR)], detour.at[a],
            send_sem.at[1], detour_sem.at[a],
            device_id={"pgroup": peers[1 - a][0]}, device_id_type=MESH,
        )

    def late_copy(a):
        rows = chunk(DETOUR)
        return pltpu.make_async_remote_copy(
            canvas.at[a, pl.ds(half, half), rows], inbox.at[pl.ds(offsets[a] + half, half), rows],
            send_sem.at[1], second_sem.at[group_of(DETOUR)],
            device_id={"pgroup": peers[a][0]}, device_id_type=MESH,
        )

    def send_first(m, a, d):
        if not (square and isinstance(m, int) and m == DETOUR):
            first_copy(m, a, d).start()
            return

        @pl.when(places[a] == 0)
        def _():
            first_copy(m, a, d).start()

        @pl.when(places[a] == 1)
        def _():
            short_copy(a).start()

        @pl.when(at_corner(a, 1, 0))
        def _():
            detour_copy(a).start()

    def arrived(view, sem):
        pltpu.make_async_copy(view, view, sem).wait()

    def put(target, a, slot, sky_tile, rows, start, terms, index, above, index_above, last, extra):
        total = sum_rows(a, terms, index, start, rows.size)
        if extra is not None:
            total = total + extra[a, slot, rows]
        target[a, slot, rows] = total
        if start == 0:
            top = total[:8] + sum_rows(a, above, index_above, BLOCK, 8)
            if last:
                top = top + halo_in[a, sky_tile]
            target[a, slot, pl.ds(rows.start, 8)] = top

    def cover(target, which, rows, sky_block, start, arrays, chips, last, extra):
        terms = block_terms(sky_block)
        above = block_terms(sky_block - 1) if start == 0 else None

        def one(n, _):
            chip_at = chips(n)
            for q in range(half):
                sky_tile = chip_at * own + which * half + q
                index = indices(terms, sky_tile)
                index_above = indices(above, sky_tile) if start == 0 else None
                for a in arrays:
                    put(
                        target, a, slot_of(a, chip_at) + q, sky_tile, rows, start,
                        terms, index, above, index_above, last, extra,
                    )
            return 0

        return one

    def part(target, which, rows, start, a, d, extra):
        at = place_of(a, d)
        chips = (lambda n: n * nx + at) if a == 0 else (lambda n: at * nx + n)
        one = cover(target, which, rows, TILE_BLOCKS - 1, start, (a,), chips, False, extra)
        lax.fori_loop(0, counts[1 - a], one, 0)

    def begin(m):
        for n, (a, d) in enumerate(remote):
            part(give, 1 - core, chunk(m), BLOCK - EARLY[m][0], a, d, None)
            swap_part(m, n).start()

    def release(m):
        if m:
            arrived(take.at[:, pl.ds(0, parts_tiles), chunk(m)], swap_sem.at[parts + m - 1])
        for n, (a, d) in enumerate(remote):
            if m == 0:
                swap_part(m, n).wait_recv()
            part(canvas, core, chunk(m), BLOCK - EARLY[m][0], a, d, take)
            send_first(m, a, d)

    def home(target, which, extra):
        if extra is not None:
            both = pl.ds(0, (sizes[0] + sizes[1]) // 2)
            arrived(take.at[:, both, pl.ds(sky_rows - BLOCK, BLOCK)], swap_sem.at[parts + FINE - 1])
        for a in range(2):
            for start in range(0, BLOCK, STEP):
                part(target, which, pl.ds(sky_rows - BLOCK + start, STEP), start, a, 0, extra)
            if extra is None:
                swap_home(a).start()

    def build(m, sky_block, start, last=False):
        one = cover(give, 1 - core, chunk(m), sky_block, start, (0, 1), lambda n: n, last, None)
        lax.fori_loop(0, ny * nx, one, 0)
        swap_all(m).start()

    def combine(m, sky_block, start, last=False):
        swap_all(m).wait_recv()
        one = cover(canvas, core, chunk(m), sky_block, start, (0, 1), lambda n: n, last, take)
        lax.fori_loop(0, ny * nx, one, 0)
        for a, d in remote:
            first_copy(m, a, d).start()

    halo = pltpu.make_async_remote_copy(
        halo_out, halo_in, halo_sem.at[0], halo_sem.at[1],
        device_id={"tile": after}, device_id_type=MESH,
    )

    top = TILE_BLOCKS - 1
    top_terms = block_terms(top)

    def border(sky_tile, _):
        index = indices(top_terms, sky_tile)
        for a in range(2):
            halo_out[a, sky_tile] = sum_rows(a, top_terms, index, BLOCK, 8)
        return 0

    bottom = blocks - 1
    loaded(0)
    interpolate(bottom, 104, 128, 3)
    pl.semaphore_wait(barrier, len(near) + jnp.where(tile > 0, 1, 0))
    begin(0)

    @pl.when(tile > 0)
    def _():
        pl.semaphore_signal(entered, inc=1, device_id={"tile": before}, device_id_type=MESH)

    @pl.when(tile == 0)
    def _():
        halo_in[...] = jnp.zeros(halo_in.shape, F32)

    loaded(1)
    interpolate(bottom, 80, 104, 3)
    begin(1)
    release(0)
    loaded(2)
    interpolate(bottom, 56, 80, 3)
    release(1)
    begin(2)
    interpolate(bottom, 0, 56, 7)
    release(2)
    for k, b in enumerate(reversed(range(blocks - 1))):
        loaded(len(PIECES) + k)
        interpolate(b, 112, 128, 2)
    begin(3)
    for b in reversed(range(blocks - 1)):
        interpolate(b, 40, 112, 3)
    release(3)
    for b in reversed(range(blocks - 1)):
        interpolate(b, 0, 40, 5)
    build(FINE, top - 1, STEP)
    home(give, 1 - core, None)
    lax.fori_loop(0, sky_tiles, border, 0, unroll=4)

    @pl.when(tile < n_tile - 1)
    def _():
        pl.semaphore_wait(entered, 1)
        halo.start()

    for i in range(top - 1):
        at = top - 1 - i
        build(FINE + 1 + 2 * i, at, 0)
        combine(FINE + 2 * i, at, STEP)
        build(FINE + 2 + 2 * i, at - 1, STEP)
        combine(FINE + 1 + 2 * i, at, 0)

    @pl.when(tile > 0)
    def _():
        halo.wait_recv()

    build(chunks - 1, 0, 0, last=True)
    combine(chunks - 2, 0, STEP)
    combine(chunks - 1, 0, 0, last=True)
    home(canvas, core, take)

    def every(step):
        for m in range(chunks):
            step(m)

    def middle(m):
        rows = chunk(m)
        bent = square and m == DETOUR
        if bent:
            for n in range(3):
                @pl.when(x + y == n)
                def _():
                    arrived(inbox.at[pl.ds(0, (2 + n) * half), rows], first_sem.at[group_of(m)])
        elif opens(m):
            arrived(inbox.at[pl.ds(0, first_tiles), group_rows(m)], first_sem.at[group_of(m)])
        for a in range(2):
            for e in range(1, counts[1 - a]):
                at = place_of(1 - a, e) * half

                def one(q, _):
                    slot = place_of(a, 0) * sizes[a] + at + q
                    total = canvas[a, slot, rows]
                    for d in range(counts[a] - 1):
                        total = total + inbox[offsets[a] + d * sizes[a] + at + q, rows]
                    canvas[a, slot, rows] = total
                    return 0

                if bent:
                    @pl.when(~at_corner(a, 0, 0))
                    def _():
                        lax.fori_loop(0, half, one, 0, unroll=True)
                else:
                    lax.fori_loop(0, half, one, 0, unroll=True)
                second_copy(m, a, e).start()
            if bent:
                @pl.when(at_corner(a, 1, 1))
                def _():
                    arrived(detour.at[a], detour_sem.at[a])
                    for q in range(half):
                        canvas[a, half + q, rows] += detour[a, q]
                    late_copy(a).start()

    every(middle)

    def finish(m):
        rows = chunk(m)
        second_count = every_tile - first_tiles
        if square and m == DETOUR:
            @pl.when(x == y)
            def _():
                arrived(inbox.at[pl.ds(0, second_count), rows], second_sem.at[group_of(m)])

            @pl.when(x != y)
            def _():
                arrived(inbox.at[pl.ds(0, second_count + half), rows], second_sem.at[group_of(m)])
        elif opens(m):
            arrived(inbox.at[pl.ds(first_tiles, second_count), group_rows(m)], second_sem.at[group_of(m)])
        for q in range(half):
            sums = []
            for a in range(2):
                at = places[1 - a] * half + q
                total = canvas[a, place_of(a, 0) * sizes[a] + at, rows]
                for d in range(counts[a] - 1):
                    total = total + inbox[offsets[a] + d * sizes[a] + at, rows]
                for e in range(counts[1 - a] - 1):
                    total = total + inbox[second_tiles[a] + e * half + q, rows]
                sums.append(total)
            lanes = slice(q * LANES, (q + 1) * LANES)
            numer[rows, lanes] = sums[0]
            weight[rows, lanes] = sums[1]
            normalised[rows, lanes] = sums[0] / jnp.maximum(sums[1], 0.05)

    every(finish)
    arrived(give, send_sem.at[0])
    arrived(inbox, send_sem.at[1])

    @pl.when(tile < n_tile - 1)
    def _():
        halo.wait_send()


def copy_out(numer, weight, normalised, numer_out, weight_out, normalised_out, sem):
    pairs = ((numer, numer_out), (weight, weight_out), (normalised, normalised_out))
    copies = [pltpu.make_async_copy(a, b, sem.at[n]) for n, (a, b) in enumerate(pairs)]
    for copy in copies:
        copy.start()
    for copy in copies:
        copy.wait()


def body(ny, nx, n_tile, images, beams, row_block, col_block, band, row_frac, col_frac):
    points, img_rows, width = images.shape
    blocks = img_rows // BLOCK
    col_tiles = width // LANES
    sky_tiles = SKY_COLS // LANES
    sky_rows = TILE_BLOCKS * BLOCK
    half = sky_tiles // (2 * ny * nx)
    per_core = sky_tiles // 2
    chunks = len(EARLY) + (TILE_BLOCKS - 1) * (BLOCK // STEP)
    own_cols = half * LANES
    inbox_tiles = (nx - 1) * (ny + 1) * half + (ny - 1) * (nx + 1) * half
    dma = pltpu.SemaphoreType.DMA
    anywhere = pl.BlockSpec(memory_space=pl.ANY)
    scalars = [pltpu.SMEM(v.shape, v.dtype) for v in (row_block, col_block, band, row_frac, col_frac)]
    vmem = pl.BlockSpec(memory_space=pltpu.VMEM)
    out = pltpu.VMEM((sky_rows, own_cols), F32)
    numer, weight, normalised = pl.pallas_call(
        functools.partial(kernel, ny, nx, n_tile),
        out_shape=(out, out, out),
        in_specs=[anywhere] * 7,
        out_specs=(vmem, vmem, vmem),
        scratch_shapes=scalars + [
            pltpu.VMEM((2, points, img_rows, width), F32),
            pltpu.VMEM((2, points * blocks * col_tiles + 1, BLOCK + 2 * PAD, LANES), F32),
            pltpu.VMEM((2, sky_tiles, 8, LANES), F32),
            pltpu.VMEM((2, sky_tiles, 8, LANES), F32),
            pltpu.VMEM((2, per_core, sky_rows, LANES), F32),
            pltpu.VMEM((2, per_core, sky_rows, LANES), F32),
            pltpu.VMEM((2, per_core, sky_rows, LANES), F32),
            pltpu.VMEM((inbox_tiles, sky_rows, LANES), F32),
            pltpu.VMEM((2, half, EARLY[DETOUR][1], LANES), F32),
            dma((5,)),
            dma((len(PIECES) + blocks - 1,)),
            dma((2,)),
            pltpu.SemaphoreType.REGULAR,
            dma((nx + ny - 2 + chunks,)),
            dma((len(GROUPS),)),
            dma((len(GROUPS),)),
            dma((2,)),
            dma((2,)),
        ],
        compiler_params=pltpu.CompilerParams(
            collective_id=0, has_side_effects=True, vmem_limit_bytes=56 * 1024 * 1024
        ),
        name="combine",
    )(images, beams, row_block, col_block, band, row_frac, col_frac)
    flat = jax.ShapeDtypeStruct((sky_rows, own_cols), F32)
    return pl.pallas_call(
        copy_out,
        out_shape=(flat, flat, flat),
        in_specs=[vmem] * 3,
        out_specs=(anywhere,) * 3,
        scratch_shapes=[dma((3,))],
        name="copy_out",
    )(*[pltpu.with_memory_space_constraint(v, pltpu.VMEM) for v in (numer, weight, normalised)])


def solution(mesh):
    ny, nx = chip_grid(mesh.shape["pgroup"])
    return jax.shard_map(
        functools.partial(body, ny, nx, mesh.shape["tile"]),
        mesh=mesh,
        in_specs=(
            P(("pgroup", "tile"), None, None),
            P(("pgroup", "tile"), None, None),
            P(("pgroup", "tile")),
            P(("pgroup", "tile")),
            P(("pgroup", "tile"), None),
            P(("pgroup", "tile")),
            P(("pgroup", "tile")),
        ),
        out_specs=(P("tile", "pgroup"), P("tile", "pgroup"), P("tile", "pgroup")),
        check_vma=False,
    )
```
